16 devices in a mesh: dp: 2 (over y, z), tp: 8 (over x, core).
Axes of the slice: x: 4, y: 2, z: 1, core: 2. Of those that a mesh axis runs over, the one named last changes fastest.
The devices are a block of a 4x4x8 slice.
Arguments:
- hidden: bfloat16 [320, 512], P('dp'), parts along dimension 0
- positions: int32 [320], P('dp'), parts along dimension 0
- self_keys: bfloat16 [2, 320, 448, 8, 64], P(None, 'dp', None, 'tp'), parts along dimension 1
- self_vals: bfloat16 [2, 320, 448, 8, 64], P(None, 'dp', None, 'tp'), parts along dimension 1
- cross_keys: bfloat16 [2, 64, 1500, 8, 64], P(None, 'dp', None, 'tp'), parts along dimension 1
- cross_vals: bfloat16 [2, 64, 1500, 8, 64], P(None, 'dp', None, 'tp'), parts along dimension 1
- ln_gain: bfloat16 [2, 3, 512], replicated
- ln_bias: bfloat16 [2, 3, 512], replicated
- w_query: bfloat16 [2, 512, 512], P(None, None, 'tp')
- b_query: bfloat16 [2, 512], P(None, 'tp')
- w_key: bfloat16 [2, 512, 512], P(None, None, 'tp')
- w_value: bfloat16 [2, 512, 512], P(None, None, 'tp')
- b_value: bfloat16 [2, 512], P(None, 'tp')
- w_out: bfloat16 [2, 512, 512], P(None, 'tp')
- b_out: bfloat16 [2, 512], replicated
- w_cquery: bfloat16 [2, 512, 512], P(None, None, 'tp')
- b_cquery: bfloat16 [2, 512], P(None, 'tp')
- w_cout: bfloat16 [2, 512, 512], P(None, 'tp')
- b_cout: bfloat16 [2, 512], replicated
- w_fc1: bfloat16 [2, 512, 2048], P(None, None, 'tp')
- b_fc1: bfloat16 [2, 2048], P(None, 'tp')
- w_fc2: bfloat16 [2, 2048, 512], P(None, 'tp')
- b_fc2: bfloat16 [2, 512], replicated
Outputs:
- output 1: bfloat16 [320, 512], P('dp'), parts along dimension 0
- output 2: bfloat16 [2, 320, 448, 8, 64], P(None, 'dp', None, 'tp'), parts along dimension 1
- output 3: bfloat16 [2, 320, 448, 8, 64], P(None, 'dp', None, 'tp'), parts along dimension 1
There are 2 independent parts. The reference program is written for one: setup_inputs(seed, part) draws one part's arguments, and reference() takes and returns one part's arrays. A program takes and returns all parts, laid end to end along the dimension named above; an argument that names none is the same for every part.
All inputs are finite; a program needn't handle non-finite values.
Results may differ from the reference program's by a relative error of at most 0.02.
Values are sent between devices in bfloat16 or wider.
A program may use at most 768 MiB of HBM per device.

```python
import jax
import jax.numpy as jnp
from jax import lax

D = 512
HEADS = 8
HEAD = 64
FF = 2048
FRAMES = 1500
CTX = 448
BEAMS = 5
AUDIOS = 32
LAYERS = 2

BATCH = AUDIOS * BEAMS
QK_SCALE = HEAD ** -0.25
EPS = 1e-5


def setup_inputs(seed: int = 0, part: int = 0) -> dict:
    part_keys = jax.random.split(jax.random.fold_in(jax.random.key(seed), part), 6)
    shared_keys = jax.random.split(jax.random.key(seed + 1), 17)

    def draw_array(key, shape, scale, offset=0.0):
        return (offset + scale * jax.random.normal(key, shape, jnp.float32)).astype(jnp.bfloat16)

    audio_pos = jax.random.randint(part_keys[1], (AUDIOS,), 3, CTX - 7)
    positions = jnp.repeat(audio_pos, BEAMS).astype(jnp.int32)
    cache_shape = (LAYERS, BATCH, CTX, HEADS, HEAD)
    cross_shape = (LAYERS, AUDIOS, FRAMES, HEADS, HEAD)
    width_scale = D ** -0.5
    return {
        'hidden': draw_array(part_keys[0], (BATCH, D), 1.0),
        'positions': positions,
        'self_keys': draw_array(part_keys[2], cache_shape, 0.3),
        'self_vals': draw_array(part_keys[3], cache_shape, 1.0),
        'cross_keys': draw_array(part_keys[4], cross_shape, 1.0),
        'cross_vals': draw_array(part_keys[5], cross_shape, 1.0),
        'ln_gain': draw_array(shared_keys[0], (LAYERS, 3, D), 0.3, 1.0),
        'ln_bias': draw_array(shared_keys[1], (LAYERS, 3, D), 0.3),
        'w_query': draw_array(shared_keys[2], (LAYERS, D, D), width_scale),
        'b_query': draw_array(shared_keys[3], (LAYERS, D), 0.3),
        'w_key': draw_array(shared_keys[4], (LAYERS, D, D), 2.0 * width_scale),
        'w_value': draw_array(shared_keys[5], (LAYERS, D, D), width_scale),
        'b_value': draw_array(shared_keys[6], (LAYERS, D), 1.0),
        'w_out': draw_array(shared_keys[7], (LAYERS, D, D), width_scale),
        'b_out': draw_array(shared_keys[8], (LAYERS, D), 0.3),
        'w_cquery': draw_array(shared_keys[9], (LAYERS, D, D), width_scale),
        'b_cquery': draw_array(shared_keys[10], (LAYERS, D), 0.3),
        'w_cout': draw_array(shared_keys[11], (LAYERS, D, D), width_scale),
        'b_cout': draw_array(shared_keys[12], (LAYERS, D), 0.3),
        'w_fc1': draw_array(shared_keys[13], (LAYERS, D, FF), width_scale),
        'b_fc1': draw_array(shared_keys[14], (LAYERS, FF), 0.3),
        'w_fc2': draw_array(shared_keys[15], (LAYERS, FF, D), FF ** -0.5),
        'b_fc2': draw_array(shared_keys[16], (LAYERS, D), 0.3),
    }


def layer_norm(values, gain_row, bias_row):
    wide_vals = values.astype(jnp.float32)
    center = wide_vals - jnp.mean(wide_vals, axis=-1, keepdims=True)
    var_est = jnp.mean(center * center, axis=-1, keepdims=True)
    return (center * lax.rsqrt(var_est + EPS) * gain_row.astype(jnp.float32) + bias_row.astype(jnp.float32)).astype(jnp.bfloat16)


def project(normed, weight, bias_row):
    return jnp.dot(normed, weight, preferred_element_type=jnp.float32) + bias_row.astype(jnp.float32)


def reference(hidden, positions, self_keys, self_vals, cross_keys, cross_vals, ln_gain, ln_bias, w_query, b_query, w_key, w_value, b_value, w_out, b_out, w_cquery, b_cquery, w_cout, b_cout, w_fc1, b_fc1, w_fc2, b_fc2):
    slot_ids = jnp.arange(CTX)[None, :]
    slot_hit = (slot_ids == positions[:, None])[:, :, None, None]
    slot_mask = (slot_ids <= positions[:, None])[:, None, :]

    def one_layer(hidden_in, layer_w):
        normed = layer_norm(hidden_in, layer_w['ln_gain'][0], layer_w['ln_bias'][0])
        query_heads = (project(normed, layer_w['w_query'], layer_w['b_query']) * QK_SCALE).astype(jnp.bfloat16).reshape(BATCH, HEADS, HEAD)
        new_key = (jnp.dot(normed, layer_w['w_key'], preferred_element_type=jnp.float32) * QK_SCALE).astype(jnp.bfloat16).reshape(BATCH, 1, HEADS, HEAD)
        new_val = project(normed, layer_w['w_value'], layer_w['b_value']).astype(jnp.bfloat16).reshape(BATCH, 1, HEADS, HEAD)
        cache_k = jnp.where(slot_hit, new_key, layer_w['cache_k'])
        cache_v = jnp.where(slot_hit, new_val, layer_w['cache_v'])
        raw_scores = jnp.einsum('bhd,bshd->bhs', query_heads.astype(jnp.float32), cache_k.astype(jnp.float32))
        attn_probs = jax.nn.softmax(jnp.where(slot_mask, raw_scores, -1e30), axis=-1).astype(jnp.bfloat16)
        attn_out = jnp.einsum('bhs,bshd->bhd', attn_probs.astype(jnp.float32), cache_v.astype(jnp.float32)).astype(jnp.bfloat16).reshape(BATCH, HEADS * HEAD)
        hidden_mid = (hidden_in.astype(jnp.float32) + project(attn_out, layer_w['w_out'], layer_w['b_out'])).astype(jnp.bfloat16)

        normed = layer_norm(hidden_mid, layer_w['ln_gain'][1], layer_w['ln_bias'][1])
        cross_query = (project(normed, layer_w['w_cquery'], layer_w['b_cquery']) * QK_SCALE).astype(jnp.bfloat16).reshape(AUDIOS, BEAMS, HEADS, HEAD)
        cross_scores = jnp.einsum('abhd,afhd->abhf', cross_query.astype(jnp.float32), layer_w['cross_k'].astype(jnp.float32))
        cross_probs = jax.nn.softmax(cross_scores, axis=-1).astype(jnp.bfloat16)
        cross_out = jnp.einsum('abhf,afhd->abhd', cross_probs.astype(jnp.float32), layer_w['cross_v'].astype(jnp.float32)).astype(jnp.bfloat16).reshape(BATCH, HEADS * HEAD)
        hidden_mid = (hidden_mid.astype(jnp.float32) + project(cross_out, layer_w['w_cout'], layer_w['b_cout'])).astype(jnp.bfloat16)

        normed = layer_norm(hidden_mid, layer_w['ln_gain'][2], layer_w['ln_bias'][2])
        mlp_inner = jax.nn.gelu(project(normed, layer_w['w_fc1'], layer_w['b_fc1']), approximate=False).astype(jnp.bfloat16)
        hidden_next = (hidden_mid.astype(jnp.float32) + project(mlp_inner, layer_w['w_fc2'], layer_w['b_fc2'])).astype(jnp.bfloat16)
        return hidden_next, (cache_k, cache_v)

    layer_stack = {'cache_k': self_keys, 'cache_v': self_vals, 'cross_k': cross_keys, 'cross_v': cross_vals, 'ln_gain': ln_gain, 'ln_bias': ln_bias, 'w_query': w_query, 'b_query': b_query, 'w_key': w_key, 'w_value': w_value, 'b_value': b_value, 'w_out': w_out, 'b_out': b_out, 'w_cquery': w_cquery, 'b_cquery': b_cquery, 'w_cout': w_cout, 'b_cout': b_cout, 'w_fc1': w_fc1, 'b_fc1': b_fc1, 'w_fc2': w_fc2, 'b_fc2': b_fc2}
    hidden_out, cache_pair = lax.scan(one_layer, hidden, layer_stack)
    return hidden_out, cache_pair[0], cache_pair[1]
```

```python
import functools

import jax
import jax.numpy as jnp
from jax import lax
from jax.experimental import pallas as pl
from jax.experimental.pallas import tpu as pltpu
from jax.sharding import PartitionSpec as P

EPS = 1e-5
NEG = -1e30
PARAM_NAMES = ('ln_gain', 'ln_bias', 'w_query', 'b_query', 'w_key', 'w_value', 'b_value', 'w_out', 'b_out', 'w_cquery', 'b_cquery', 'w_cout', 'b_cout', 'w_fc1', 'b_fc1', 'w_fc2', 'b_fc2')
F32 = jnp.float32
BF16 = jnp.bfloat16
VMEM = pltpu.VMEM
NT = (((1,), (1,)), ((), ()))


def dot(a, b):
    return jnp.dot(a, b, preferred_element_type=F32)


def dot_nt(a, b):
    return lax.dot_general(a, b, NT, preferred_element_type=F32)


def layer_norm(wide_vals, gain_row, bias_row):
    center = wide_vals - jnp.mean(wide_vals, axis=-1, keepdims=True)
    var_est = jnp.mean(center * center, axis=-1, keepdims=True)
    return (center * lax.rsqrt(var_est + EPS) * gain_row + bias_row).astype(BF16)


def iota(shape, dim):
    return lax.broadcasted_iota(jnp.int32, shape, dim)


def stack_eye(rows, width):
    return (iota((width, rows), 1) % width == iota((width, rows), 0)).astype(BF16)


def row(ref, *idx):
    return ref[idx].astype(F32)


def self_kernel(layer, group, pos_ref, hidden_ref, gain_ref, bias_ref, wq_ref, bq_ref, wk_ref, wv_ref, bv_ref, kin_ref, vin_ref, *rest):
    o_ref, kout_ref, vout_ref, kbuf, vbuf, qbd, kcol, vcol, osc, in_sem, out_sem = rest[-11:]
    batch = hidden_ref.shape[0]
    head = wq_ref.shape[1]
    slots = kbuf.shape[2]
    groups = batch // group
    span = group * head
    base = layer * batch * head
    scale = head ** -0.25

    def in_copy(src, buf, which, g):
        return pltpu.make_async_copy(src.at[pl.ds(base + g * span, span), :], buf.at[g], in_sem.at[which, g])

    def out_copy(buf, dst, which, g):
        return pltpu.make_async_copy(buf.at[g], dst.at[pl.ds(base + g * span, span), :], out_sem.at[which, g])

    def start(g, carry):
        in_copy(kin_ref, kbuf, 0, g).start()
        in_copy(vin_ref, vbuf, 1, g).start()
        return carry

    lax.fori_loop(0, groups, start, 0)

    normed = layer_norm(hidden_ref[...].astype(F32), gain_ref[0, layer:layer + 1, :].astype(F32), bias_ref[0, layer:layer + 1, :].astype(F32))
    q = ((dot_nt(normed, wq_ref[layer]) + bq_ref[layer:layer + 1, :].astype(F32)) * scale).astype(BF16)
    k = (dot_nt(normed, wk_ref[layer]) * scale).astype(BF16)
    v = (dot_nt(normed, wv_ref[layer]) + bv_ref[layer:layer + 1, :].astype(F32)).astype(BF16)
    eye = stack_eye(span, head)
    wide_q = dot(q, eye)
    diag = iota((batch, span), 0) % group == iota((batch, span), 1) // head
    qbd[...] = jnp.where(diag, wide_q, 0.0)
    k_t = k.astype(F32).T
    v_t = v.astype(F32).T
    for g in range(groups):
        kcol[g] = k_t[:, g * group:(g + 1) * group]
        vcol[g] = v_t[:, g * group:(g + 1) * group]

    lane_ids = iota((group, slots), 1)
    row_ids = iota((group, slots), 0)
    odiag = iota((span, group), 0) // head == iota((span, group), 1)
    full_tiles = slots // 128
    tail = slots - full_tiles * 128

    def attend(g, carry):
        in_copy(kin_ref, kbuf, 0, g).wait()
        in_copy(vin_ref, vbuf, 1, g).wait()
        kc = kcol[g]
        vc = vcol[g]
        limit = jnp.zeros((group, slots), jnp.int32)
        for i in range(group):
            pos = pos_ref[g * group + i]
            limit = jnp.where(row_ids == i, pos, limit)
            tile = pos // 128
            local = pos - tile * 128
            rows = slice(i * head, (i + 1) * head)

            def put(cols, width):
                hit = iota((head, width), 1) == local
                for buf, col in ((kbuf, kc), (vbuf, vc)):
                    old = buf[g, rows, cols].astype(F32)
                    buf[g, rows, cols] = jnp.where(hit, col[:, i:i + 1], old).astype(BF16)

            @pl.when(tile < full_tiles)
            def _():
                put(pl.ds(pl.multiple_of(tile * 128, 128), 128), 128)

            @pl.when(tile >= full_tiles)
            def _():
                put(slice(full_tiles * 128, slots), tail)

        out_copy(kbuf, kout_ref, 0, g).start()
        out_copy(vbuf, vout_ref, 1, g).start()
        scores = dot(qbd[pl.ds(pl.multiple_of(g * group, group), group), :].astype(BF16), kbuf[g])
        scores = jnp.where(lane_ids <= limit, scores, NEG)
        probs = jnp.exp(scores - jnp.max(scores, axis=-1, keepdims=True))
        probs = (probs / jnp.sum(probs, axis=-1, keepdims=True)).astype(BF16)
        wide_o = dot_nt(vbuf[g], probs)
        o_t = dot(eye, jnp.where(odiag, wide_o, 0.0).astype(BF16))
        osc[pl.ds(pl.multiple_of(g * group, group), group), :] = o_t.T
        return carry

    lax.fori_loop(0, groups, attend, 0)
    o_ref[...] = osc[...].astype(BF16)

    def finish(g, carry):
        out_copy(kbuf, kout_ref, 0, g).wait()
        out_copy(vbuf, vout_ref, 1, g).wait()
        return carry

    lax.fori_loop(0, groups, finish, 0)


def self_attention(layer, hidden, positions, keys, vals, prev, params):
    batch = hidden.shape[0]
    head = params['w_query'].shape[1]
    slots = keys.shape[1]
    group = 8
    groups = batch // group
    any_spec = pl.BlockSpec(memory_space=pltpu.HBM)
    vm = pl.BlockSpec(memory_space=VMEM)
    operands = [positions, hidden, params['ln_gain'], params['ln_bias'], params['w_query'], params['b_query'], params['w_key'], params['w_value'], params['b_value'], keys, vals]
    in_specs = [pl.BlockSpec(memory_space=pltpu.SMEM)] + [vm] * 8 + [any_spec] * 2
    aliases = {}
    if prev is not None:
        operands += list(prev)
        in_specs += [any_spec] * 2
        aliases = {11: 1, 12: 2}
    return pl.pallas_call(
        functools.partial(self_kernel, layer, group),
        out_shape=(jax.ShapeDtypeStruct((batch, head), BF16), jax.ShapeDtypeStruct(keys.shape, BF16), jax.ShapeDtypeStruct(vals.shape, BF16)),
        in_specs=in_specs,
        out_specs=(vm, any_spec, any_spec),
        scratch_shapes=[
            VMEM((groups, group * head, slots), BF16),
            VMEM((groups, group * head, slots), BF16),
            VMEM((batch, group * head), F32),
            VMEM((groups, head, group), F32),
            VMEM((groups, head, group), F32),
            VMEM((batch, head), F32),
            pltpu.SemaphoreType.DMA((2, groups)),
            pltpu.SemaphoreType.DMA((2, groups)),
        ],
        input_output_aliases=aliases,
        compiler_params=pltpu.CompilerParams(vmem_limit_bytes=40 * 2**20),
        name='self_attention',
    )(*operands)


def cross_kernel(layer, tp, group, o_ref, hidden_ref, gain_ref, bias_ref, wo_ref, bo_ref, wcq_ref, bcq_ref, wco_ref, bco_ref, w1_ref, b1_ref, w2_ref, b2_ref, kin_ref, vin_ref, hidden_out_ref, kbuf, vbuf, part, landed, blocks, qbd, osc, in_sem, rs_send, rs_recv, ag_send, ag_recv):
    me = lax.axis_index('tp')
    batch, width = hidden_ref.shape
    head = wcq_ref.shape[1]
    half = batch // 2
    quarters = width // 128
    chunks = kbuf.shape[0]
    span = kbuf.shape[1]
    base = layer * chunks * span
    scale = head ** -0.25
    beams = batch // (chunks * group)
    rows = group * beams

    def in_copy(src, buf, which, c):
        return pltpu.make_async_copy(src.at[pl.ds(base + c * span, span), :], buf.at[c], in_sem.at[which, c])

    for c in range(chunks):
        in_copy(kin_ref, kbuf, 0, c).start()
        in_copy(vin_ref, vbuf, 1, c).start()

    barrier = pltpu.get_barrier_semaphore()
    peers = [lax.rem(me + step, tp) for step in range(1, tp)]
    for peer in peers:
        pl.semaphore_signal(barrier, inc=1, device_id={'tp': peer}, device_id_type=pl.DeviceIdType.MESH)

    def bounds(j):
        r, c = j // quarters, j % quarters
        return slice(r * half, (r + 1) * half), slice(c * 128, (c + 1) * 128)

    for j in range(tp):
        rs, cs = bounds(j)
        blocks[0, j] = hidden_ref[rs, cs]

    def exchange(x, total, bias_ref, entry):
        for j in range(tp):
            rs, cs = bounds(j)
            part[x, j] = total[rs, cs].astype(BF16)
        if entry:
            pl.semaphore_wait(barrier, tp - 1)
        sends = []
        for n, peer in enumerate(peers):
            copy = pltpu.make_async_remote_copy(part.at[x, peer], landed.at[x, me], rs_send.at[x, n], rs_recv.at[x, me], device_id={'tp': peer}, device_id_type=pl.DeviceIdType.MESH)
            copy.start()
            sends.append(copy)
        bias = bias_ref[layer:layer + 1, :].astype(F32)
        own = lax.rem(me, quarters)
        bias_row = jnp.zeros((1, 128), F32)
        for c in range(quarters):
            bias_row = jnp.where(own == c, bias[:, c * 128:(c + 1) * 128], bias_row)
        acc = part[x, me].astype(F32)
        for peer in reversed(peers):
            pltpu.make_async_remote_copy(part.at[x, peer], landed.at[x, peer], rs_send.at[x, 0], rs_recv.at[x, peer], device_id={'tp': peer}, device_id_type=pl.DeviceIdType.MESH).wait_recv()
            acc = acc + landed[x, peer].astype(F32)
        blocks[x + 1, me] = (blocks[x, me].astype(F32) + acc + bias_row).astype(BF16)
        for n, peer in enumerate(peers):
            copy = pltpu.make_async_remote_copy(blocks.at[x + 1, me], blocks.at[x + 1, me], ag_send.at[x, n], ag_recv.at[x, me], device_id={'tp': peer}, device_id_type=pl.DeviceIdType.MESH)
            copy.start()
            sends.append(copy)
        for peer in peers:
            pltpu.make_async_remote_copy(blocks.at[x + 1, peer], blocks.at[x + 1, peer], ag_send.at[x, 0], ag_recv.at[x, peer], device_id={'tp': peer}, device_id_type=pl.DeviceIdType.MESH).wait_recv()
        for copy in sends:
            copy.wait_send()

    def whole(x):
        tops = [jnp.concatenate([blocks[x, r * quarters + c] for c in range(quarters)], axis=1) for r in range(tp // quarters)]
        return jnp.concatenate(tops, axis=0)

    exchange(0, dot(o_ref[...], wo_ref[layer]), bo_ref, True)

    normed = layer_norm(whole(1).astype(F32), gain_ref[1, layer:layer + 1, :].astype(F32), bias_ref[1, layer:layer + 1, :].astype(F32))
    q = ((dot_nt(normed, wcq_ref[layer]) + bcq_ref[layer:layer + 1, :].astype(F32)) * scale).astype(BF16)
    eye = stack_eye(span, head)
    diag = (iota((batch, span), 0) // beams) % group == iota((batch, span), 1) // head
    qbd[...] = jnp.where(diag, dot(q, eye), 0.0)
    odiag = iota((span, rows), 0) // head == iota((span, rows), 1) // beams
    for c in range(chunks):
        in_copy(kin_ref, kbuf, 0, c).wait()
        scores = dot(qbd[c * rows:(c + 1) * rows, :].astype(BF16), kbuf[c])
        probs = jnp.exp(scores - jnp.max(scores, axis=-1, keepdims=True))
        probs = (probs / jnp.sum(probs, axis=-1, keepdims=True)).astype(BF16)
        in_copy(vin_ref, vbuf, 1, c).wait()
        wide_o = dot_nt(vbuf[c], probs)
        o_t = dot(eye, jnp.where(odiag, wide_o, 0.0).astype(BF16))
        osc[c * rows:(c + 1) * rows, :] = o_t.T
    exchange(1, dot(osc[...].astype(BF16), wco_ref[layer]), bco_ref, False)

    normed = layer_norm(whole(2).astype(F32), gain_ref[2, layer:layer + 1, :].astype(F32), bias_ref[2, layer:layer + 1, :].astype(F32))
    inner = dot(normed, w1_ref[layer]) + b1_ref[layer:layer + 1, :].astype(F32)
    inner = (0.5 * inner * (1.0 + lax.erf(inner * (0.5 ** 0.5)))).astype(BF16)
    exchange(2, dot(inner, w2_ref[layer]), b2_ref, False)
    hidden_out_ref[...] = whole(3)


def cross_and_mlp(layer, tp, attn_out, hidden, keys, vals, audios, params):
    batch, width = hidden.shape
    head = params['w_cquery'].shape[1]
    frames = keys.shape[1]
    group = 8
    chunks = audios // group
    vm = pl.BlockSpec(memory_space=VMEM)
    any_spec = pl.BlockSpec(memory_space=pltpu.HBM)
    names = ('ln_gain', 'ln_bias', 'w_out', 'b_out', 'w_cquery', 'b_cquery', 'w_cout', 'b_cout', 'w_fc1', 'b_fc1', 'w_fc2', 'b_fc2')
    block = (batch // 2, 128)
    return pl.pallas_call(
        functools.partial(cross_kernel, layer, tp, group),
        out_shape=jax.ShapeDtypeStruct((batch, width), BF16),
        in_specs=[vm] * 14 + [any_spec] * 2,
        out_specs=vm,
        scratch_shapes=[
            VMEM((chunks, group * head, frames), BF16),
            VMEM((chunks, group * head, frames), BF16),
            VMEM((3, tp) + block, BF16),
            VMEM((3, tp) + block, BF16),
            VMEM((4, tp) + block, BF16),
            VMEM((batch, group * head), F32),
            VMEM((batch, head), F32),
            pltpu.SemaphoreType.DMA((2, chunks)),
            pltpu.SemaphoreType.DMA((3, tp - 1)),
            pltpu.SemaphoreType.DMA((3, tp)),
            pltpu.SemaphoreType.DMA((3, tp - 1)),
            pltpu.SemaphoreType.DMA((3, tp)),
        ],
        compiler_params=pltpu.CompilerParams(vmem_limit_bytes=40 * 2**20, collective_id=layer, has_side_effects=True),
        name='cross_and_mlp',
    )(attn_out, hidden, *[params[n] for n in names], keys, vals)


def solution(mesh):
    tp = mesh.shape['tp']
    cache_spec = P(None, 'dp', None, 'tp', None)
    col_spec = P(None, None, 'tp')
    row_spec = P(None, 'tp', None)
    vec_spec = P(None, 'tp')
    param_specs = {'ln_gain': P(), 'ln_bias': P(), 'w_query': col_spec, 'b_query': vec_spec, 'w_key': col_spec, 'w_value': col_spec, 'b_value': vec_spec, 'w_out': row_spec, 'b_out': P(), 'w_cquery': col_spec, 'b_cquery': vec_spec, 'w_cout': row_spec, 'b_cout': P(), 'w_fc1': col_spec, 'b_fc1': vec_spec, 'w_fc2': row_spec, 'b_fc2': P()}
    in_specs = (P('dp', None), P('dp'), cache_spec, cache_spec, cache_spec, cache_spec) + tuple(param_specs[param_name] for param_name in PARAM_NAMES)

    def flat(cache):
        layers, n, slots, heads, head = cache.shape
        return cache.transpose(0, 1, 3, 4, 2).reshape(layers * n * heads * head, slots)

    def local_step(hidden, positions, self_keys, self_vals, cross_keys, cross_vals, *layer_params):
        params = dict(zip(PARAM_NAMES, layer_params))
        for name in ('w_query', 'w_key', 'w_value', 'w_cquery'):
            params[name] = params[name].transpose(0, 2, 1)
        for name in ('ln_gain', 'ln_bias'):
            params[name] = params[name].transpose(1, 0, 2)
        layers, batch, slots, heads, head = self_keys.shape
        audios = cross_keys.shape[1]
        keys, vals, ckeys, cvals = flat(self_keys), flat(self_vals), flat(cross_keys), flat(cross_vals)
        prev = None
        for layer in range(layers):
            attn_out, *prev = self_attention(layer, hidden, positions, keys, vals, prev, params)
            hidden = cross_and_mlp(layer, tp, attn_out, hidden, ckeys, cvals, audios, params)

        def unflat(cache):
            return cache.reshape(layers, batch, heads, head, slots).transpose(0, 1, 4, 2, 3)

        return hidden, unflat(prev[0]), unflat(prev[1])

    return jax.shard_map(local_step, mesh=mesh, in_specs=in_specs, out_specs=(P('dp', None), cache_spec, cache_spec), check_vma=False)
```

```python
import functools

import jax
import jax.numpy as jnp
from jax import lax
from jax.experimental import pallas as pl
from jax.experimental.pallas import tpu as pltpu
from jax.sharding import PartitionSpec as P

EPS = 1e-5
NEG = -1e30
PARAM_NAMES = ('ln_gain', 'ln_bias', 'w_query', 'b_query', 'w_key', 'w_value', 'b_value', 'w_out', 'b_out', 'w_cquery', 'b_cquery', 'w_cout', 'b_cout', 'w_fc1', 'b_fc1', 'w_fc2', 'b_fc2')
F32 = jnp.float32
BF16 = jnp.bfloat16
VMEM = pltpu.VMEM
NT = (((1,), (1,)), ((), ()))


def dot(a, b):
    return jnp.dot(a, b, preferred_element_type=F32)


def dot_nt(a, b):
    return lax.dot_general(a, b, NT, preferred_element_type=F32)


def layer_norm(wide_vals, gain_row, bias_row):
    center = wide_vals - jnp.mean(wide_vals, axis=-1, keepdims=True)
    var_est = jnp.mean(center * center, axis=-1, keepdims=True)
    return (center * lax.rsqrt(var_est + EPS) * gain_row + bias_row).astype(BF16)


def iota(shape, dim):
    return lax.broadcasted_iota(jnp.int32, shape, dim)


def stack_eye(rows, width):
    return (iota((width, rows), 1) % width == iota((width, rows), 0)).astype(BF16)


def row(ref, *idx):
    return ref[idx].astype(F32)


def load_all(pairs, sem):
    copies = [pltpu.make_async_copy(src, dst, sem.at[n]) for n, (src, dst) in enumerate(pairs)]
    for copy in copies:
        copy.start()
    return copies


def self_kernel(layer, group, pos_hbm, hidden_hbm, gain_hbm, bias_hbm, wq_hbm, bq_hbm, wk_hbm, wv_hbm, bv_hbm, kin_ref, vin_ref, *rest):
    (o_ref, kout_ref, vout_ref, kbuf, vbuf, qbd, kcol, vcol, scores, osc, pos_ref, hidden_ref, gain_ref, bias_ref, wq_ref, bq_ref, wk_ref, wv_ref, bv_ref, in_sem, out_sem, param_sem) = rest[-22:]
    batch = hidden_ref.shape[0]
    head = wq_ref.shape[0]
    slots = kbuf.shape[2]
    groups = batch // group
    span = group * head
    base = layer * batch * head
    scale = head ** -0.25

    def in_copy(src, buf, which, g):
        return pltpu.make_async_copy(src.at[pl.ds(base + g * span, span), :], buf.at[g], in_sem.at[which, g])

    def out_copy(buf, dst, which, g):
        return pltpu.make_async_copy(buf.at[g], dst.at[pl.ds(base + g * span, span), :], out_sem.at[which, g])

    copies = load_all([(hidden_hbm, hidden_ref), (gain_hbm, gain_ref), (bias_hbm, bias_ref), (wq_hbm.at[layer], wq_ref), (bq_hbm, bq_ref), (wk_hbm.at[layer], wk_ref), (wv_hbm.at[layer], wv_ref), (bv_hbm, bv_ref), (pos_hbm, pos_ref)], param_sem)

    def start(g, carry):
        in_copy(kin_ref, kbuf, 0, g).start()
        in_copy(vin_ref, vbuf, 1, g).start()
        return carry

    lax.fori_loop(0, groups, start, 0)
    for copy in copies:
        copy.wait()

    normed = layer_norm(hidden_ref[...].astype(F32), gain_ref[0, layer:layer + 1, :].astype(F32), bias_ref[0, layer:layer + 1, :].astype(F32))
    q = ((dot_nt(normed, wq_ref[...]) + bq_ref[layer:layer + 1, :].astype(F32)) * scale).astype(BF16)
    k = (dot_nt(normed, wk_ref[...]) * scale).astype(BF16)
    v = (dot_nt(normed, wv_ref[...]) + bv_ref[layer:layer + 1, :].astype(F32)).astype(BF16)
    wide_q = dot(q, stack_eye(span, head))
    diag = iota((batch, span), 0) % group == iota((batch, span), 1) // head
    qbd[...] = jnp.where(diag, wide_q, 0.0)
    k_t = k.astype(F32).T
    v_t = v.astype(F32).T
    for g in range(groups):
        kcol[g] = k_t[:, g * group:(g + 1) * group]
        vcol[g] = v_t[:, g * group:(g + 1) * group]

    full_tiles = slots // 128
    tail = slots - full_tiles * 128

    def rows_of(g):
        return pl.ds(pl.multiple_of(g * group, group), group)

    def update(g):
        in_copy(kin_ref, kbuf, 0, g).wait()
        in_copy(vin_ref, vbuf, 1, g).wait()
        kc = kcol[g]
        vc = vcol[g]
        for i in range(group):
            pos = pos_ref[g * group + i]
            rows = slice(i * head, (i + 1) * head)
            first = pl.multiple_of(jnp.minimum(pos // 128, full_tiles - 1) * 128, 128)
            places = [(pl.ds(first, 128), iota((head, 128), 1) + first == pos)]
            if tail:
                places.append((slice(full_tiles * 128, slots), iota((head, tail), 1) + full_tiles * 128 == pos))
            for cols, hit in places:
                for buf, col in ((kbuf, kc), (vbuf, vc)):
                    old = buf[g, rows, cols].astype(F32)
                    buf[g, rows, cols] = jnp.where(hit, col[:, i:i + 1], old).astype(BF16)

    def score(g):
        limit = jnp.zeros((group, 1), jnp.int32)
        for i in range(group):
            limit = jnp.where(iota((group, 1), 0) == i, pos_ref[g * group + i], limit)
        raw = dot(qbd[rows_of(g), :].astype(BF16), kbuf[g])
        scores[rows_of(g), :] = jnp.where(iota((group, slots), 1) <= limit, raw, NEG)

    def write_back(g):
        out_copy(kbuf, kout_ref, 0, g).start()
        out_copy(vbuf, vout_ref, 1, g).start()

    def scan_keys(g, carry):
        score(g - 1)
        write_back(g - 1)
        update(g)
        return carry

    update(0)
    lax.fori_loop(1, groups, scan_keys, 0)
    score(groups - 1)
    write_back(groups - 1)

    raw = scores[...]
    probs = jnp.exp(raw - jnp.max(raw, axis=-1, keepdims=True))
    scores[...] = probs * (1.0 / jnp.sum(probs, axis=-1, keepdims=True))

    def weigh(g):
        wide_o = dot_nt(vbuf[g], scores[rows_of(g), :].astype(BF16))
        o_t = jnp.zeros((head, group), F32)
        for i in range(group):
            o_t = o_t + jnp.where(iota((head, group), 1) == i, wide_o[i * head:(i + 1) * head, :], 0.0)
        osc[rows_of(g), :] = o_t.T

    batch_of = 4

    def scan_vals(n, carry):
        for i in range(batch_of):
            weigh(n * batch_of + i)
        return carry

    lax.fori_loop(0, groups // batch_of, scan_vals, 0)
    o_ref[...] = osc[...].astype(BF16)

    def finish(g, carry):
        out_copy(kbuf, kout_ref, 0, g).wait()
        out_copy(vbuf, vout_ref, 1, g).wait()
        return carry

    lax.fori_loop(0, groups, finish, 0)


def in_hbm(arrays):
    return [pltpu.with_memory_space_constraint(a, pltpu.HBM) for a in arrays]


def self_attention(layer, hidden, positions, keys, vals, prev, params):
    batch = hidden.shape[0]
    head = params['w_query'].shape[1]
    slots = keys.shape[1]
    group = 8
    groups = batch // group
    hbm = pl.BlockSpec(memory_space=pltpu.HBM)
    operands = [positions, hidden, params['ln_gain'], params['ln_bias'], params['w_query'], params['b_query'], params['w_key'], params['w_value'], params['b_value'], keys, vals]
    aliases = {}
    if prev is not None:
        operands += list(prev)
        aliases = {11: 1, 12: 2}
    weight = VMEM(params['w_query'].shape[1:], BF16)
    vector = VMEM(params['b_query'].shape, BF16)
    norm = VMEM(params['ln_gain'].shape, BF16)
    return pl.pallas_call(
        functools.partial(self_kernel, layer, group),
        out_shape=(jax.ShapeDtypeStruct((batch, head), BF16), jax.ShapeDtypeStruct(keys.shape, BF16), jax.ShapeDtypeStruct(vals.shape, BF16)),
        in_specs=[hbm] * len(operands),
        out_specs=(pl.BlockSpec(memory_space=VMEM), hbm, hbm),
        scratch_shapes=[
            VMEM((groups, group * head, slots), BF16),
            VMEM((groups, group * head, slots), BF16),
            VMEM((batch, group * head), F32),
            VMEM((groups, head, group), F32),
            VMEM((groups, head, group), F32),
            VMEM((batch, slots), F32),
            VMEM((batch, head), F32),
            pltpu.SMEM((batch,), jnp.int32),
            VMEM(hidden.shape, BF16),
            norm, norm, weight, vector, weight, weight, vector,
            pltpu.SemaphoreType.DMA((2, groups)),
            pltpu.SemaphoreType.DMA((2, groups)),
            pltpu.SemaphoreType.DMA((9,)),
        ],
        input_output_aliases=aliases,
        compiler_params=pltpu.CompilerParams(vmem_limit_bytes=40 * 2**20),
        name='self_attention',
    )(*in_hbm(operands))


def cross_kernel(layer, tp, group, o_ref, hidden_hbm, *rest):
    param_hbm, (kin_ref, vin_ref, hidden_out_ref, kbuf, vbuf, part, landed, blocks, qbd, scores, osc, hidden_ref), rest = rest[:12], rest[12:24], rest[24:]
    param_refs, (param_sem, in_sem, rs_send, rs_recv, ag_send, ag_recv) = rest[:12], rest[12:]
    gain_ref, bias_ref, bo_ref, bcq_ref, bco_ref, b1_ref, b2_ref, wo_ref, wcq_ref, wco_ref, w1_ref, w2_ref = param_refs
    me = lax.axis_index('tp')
    batch, width = hidden_ref.shape
    head = wcq_ref.shape[0]
    half = batch // 2
    quarters = width // 128
    chunks = kbuf.shape[0]
    span = kbuf.shape[1]
    base = layer * chunks * span
    scale = head ** -0.25
    beams = batch // (chunks * group)
    rows = group * beams

    def in_copy(src, buf, which, c):
        return pltpu.make_async_copy(src.at[pl.ds(base + c * span, span), :], buf.at[c], in_sem.at[which, c])

    pairs = [(hidden_hbm, hidden_ref)]
    for src, dst in zip(param_hbm, param_refs):
        pairs.append((src if src.shape == dst.shape else src.at[layer], dst))
    copies = load_all(pairs, param_sem)
    for c in range(chunks):
        in_copy(kin_ref, kbuf, 0, c).start()
    for c in range(chunks):
        in_copy(vin_ref, vbuf, 1, c).start()

    barrier = pltpu.get_barrier_semaphore()
    peers = [lax.rem(me + step, tp) for step in range(1, tp)]
    for peer in peers:
        pl.semaphore_signal(barrier, inc=1, device_id={'tp': peer}, device_id_type=pl.DeviceIdType.MESH)

    for copy in copies:
        copy.wait()

    def bounds(j):
        r, c = j // quarters, j % quarters
        return slice(r * half, (r + 1) * half), slice(c * 128, (c + 1) * 128)

    for j in range(tp):
        rs, cs = bounds(j)
        blocks[0, j] = hidden_ref[rs, cs]

    def exchange(x, total, bias_ref, entry):
        for j in range(tp):
            rs, cs = bounds(j)
            part[x, j] = total[rs, cs].astype(BF16)
        if entry:
            pl.semaphore_wait(barrier, tp - 1)
        sends = []
        for n, peer in enumerate(peers):
            copy = pltpu.make_async_remote_copy(part.at[x, peer], landed.at[x, me], rs_send.at[x, n], rs_recv.at[x, me], device_id={'tp': peer}, device_id_type=pl.DeviceIdType.MESH)
            copy.start()
            sends.append(copy)
        bias = bias_ref[layer:layer + 1, :].astype(F32)
        own = lax.rem(me, quarters)
        bias_row = jnp.zeros((1, 128), F32)
        for c in range(quarters):
            bias_row = jnp.where(own == c, bias[:, c * 128:(c + 1) * 128], bias_row)
        acc = part[x, me].astype(F32)
        for peer in reversed(peers):
            pltpu.make_async_remote_copy(part.at[x, peer], landed.at[x, peer], rs_send.at[x, 0], rs_recv.at[x, peer], device_id={'tp': peer}, device_id_type=pl.DeviceIdType.MESH).wait_recv()
            acc = acc + landed[x, peer].astype(F32)
        blocks[x + 1, me] = (blocks[x, me].astype(F32) + acc + bias_row).astype(BF16)
        for n, peer in enumerate(peers):
            copy = pltpu.make_async_remote_copy(blocks.at[x + 1, me], blocks.at[x + 1, me], ag_send.at[x, n], ag_recv.at[x, me], device_id={'tp': peer}, device_id_type=pl.DeviceIdType.MESH)
            copy.start()
            sends.append(copy)
        for peer in peers:
            pltpu.make_async_remote_copy(blocks.at[x + 1, peer], blocks.at[x + 1, peer], ag_send.at[x, 0], ag_recv.at[x, peer], device_id={'tp': peer}, device_id_type=pl.DeviceIdType.MESH).wait_recv()
        for copy in sends:
            copy.wait_send()

    def whole(x):
        tops = [jnp.concatenate([blocks[x, r * quarters + c] for c in range(quarters)], axis=1) for r in range(tp // quarters)]
        return jnp.concatenate(tops, axis=0)

    exchange(0, dot(o_ref[...], wo_ref[...]), bo_ref, True)

    normed = layer_norm(whole(1).astype(F32), gain_ref[1, layer:layer + 1, :].astype(F32), bias_ref[1, layer:layer + 1, :].astype(F32))
    q = ((dot_nt(normed, wcq_ref[...]) + bcq_ref[layer:layer + 1, :].astype(F32)) * scale).astype(BF16)
    diag = (iota((batch, span), 0) // beams) % group == iota((batch, span), 1) // head
    qbd[...] = jnp.where(diag, dot(q, stack_eye(span, head)), 0.0).astype(BF16)
    for c in range(chunks):
        in_copy(kin_ref, kbuf, 0, c).wait()
        scores[c * rows:(c + 1) * rows, :] = dot(qbd[c * rows:(c + 1) * rows, :], kbuf[c])
    for c in range(chunks):
        raw = scores[c * rows:(c + 1) * rows, :]
        probs = jnp.exp(raw - jnp.max(raw, axis=-1, keepdims=True))
        probs = (probs * (1.0 / jnp.sum(probs, axis=-1, keepdims=True))).astype(BF16)
        in_copy(vin_ref, vbuf, 1, c).wait()
        wide_o = dot_nt(vbuf[c], probs)
        o_t = jnp.zeros((head, rows), F32)
        for i in range(group):
            o_t = o_t + jnp.where(iota((head, rows), 1) // beams == i, wide_o[i * head:(i + 1) * head, :], 0.0)
        osc[c * rows:(c + 1) * rows, :] = o_t.T
    exchange(1, dot(osc[...].astype(BF16), wco_ref[...]), bco_ref, False)

    normed = layer_norm(whole(2).astype(F32), gain_ref[2, layer:layer + 1, :].astype(F32), bias_ref[2, layer:layer + 1, :].astype(F32))
    inner = dot(normed, w1_ref[...]) + b1_ref[layer:layer + 1, :].astype(F32)
    inner = (0.5 * inner * (1.0 + lax.erf(inner * (0.5 ** 0.5)))).astype(BF16)
    exchange(2, dot(inner, w2_ref[...]), b2_ref, False)
    hidden_out_ref[...] = whole(3)


def cross_and_mlp(layer, tp, attn_out, hidden, keys, vals, audios, params):
    batch, width = hidden.shape
    head = params['w_cquery'].shape[1]
    frames = keys.shape[1]
    group = 8
    chunks = audios // group
    vm = pl.BlockSpec(memory_space=VMEM)
    hbm = pl.BlockSpec(memory_space=pltpu.HBM)
    vectors = ('ln_gain', 'ln_bias', 'b_out', 'b_cquery', 'b_cout', 'b_fc1', 'b_fc2')
    weights = ('w_out', 'w_cquery', 'w_cout', 'w_fc1', 'w_fc2')
    operands = [hidden] + [params[n] for n in vectors + weights] + [keys, vals]
    block = (batch // 2, 128)
    return pl.pallas_call(
        functools.partial(cross_kernel, layer, tp, group),
        out_shape=jax.ShapeDtypeStruct((batch, width), BF16),
        in_specs=[vm] + [hbm] * len(operands),
        out_specs=vm,
        scratch_shapes=[
            VMEM((chunks, group * head, frames), BF16),
            VMEM((chunks, group * head, frames), BF16),
            VMEM((3, tp) + block, BF16),
            VMEM((3, tp) + block, BF16),
            VMEM((4, tp) + block, BF16),
            VMEM((batch, group * head), BF16),
            VMEM((batch, frames), F32),
            VMEM((batch, head), F32),
            VMEM(hidden.shape, BF16),
        ] + [VMEM(params[n].shape, BF16) for n in vectors] + [VMEM(params[n].shape[1:], BF16) for n in weights] + [
            pltpu.SemaphoreType.DMA((13,)),
            pltpu.SemaphoreType.DMA((2, chunks)),
            pltpu.SemaphoreType.DMA((3, tp - 1)),
            pltpu.SemaphoreType.DMA((3, tp)),
            pltpu.SemaphoreType.DMA((3, tp - 1)),
            pltpu.SemaphoreType.DMA((3, tp)),
        ],
        compiler_params=pltpu.CompilerParams(vmem_limit_bytes=40 * 2**20, collective_id=layer, has_side_effects=True),
        name='cross_and_mlp',
    )(attn_out, *in_hbm(operands))


def solution(mesh):
    tp = mesh.shape['tp']
    cache_spec = P(None, 'dp', None, 'tp', None)
    col_spec = P(None, None, 'tp')
    row_spec = P(None, 'tp', None)
    vec_spec = P(None, 'tp')
    param_specs = {'ln_gain': P(), 'ln_bias': P(), 'w_query': col_spec, 'b_query': vec_spec, 'w_key': col_spec, 'w_value': col_spec, 'b_value': vec_spec, 'w_out': row_spec, 'b_out': P(), 'w_cquery': col_spec, 'b_cquery': vec_spec, 'w_cout': row_spec, 'b_cout': P(), 'w_fc1': col_spec, 'b_fc1': vec_spec, 'w_fc2': row_spec, 'b_fc2': P()}
    in_specs = (P('dp', None), P('dp'), cache_spec, cache_spec, cache_spec, cache_spec) + tuple(param_specs[param_name] for param_name in PARAM_NAMES)

    def flat(cache):
        layers, n, slots, heads, head = cache.shape
        return cache.transpose(0, 1, 3, 4, 2).reshape(layers * n * heads * head, slots)

    def local_step(hidden, positions, self_keys, self_vals, cross_keys, cross_vals, *layer_params):
        params = dict(zip(PARAM_NAMES, layer_params))
        for name in ('w_query', 'w_key', 'w_value', 'w_cquery'):
            params[name] = params[name].transpose(0, 2, 1)
        for name in ('ln_gain', 'ln_bias'):
            params[name] = params[name].transpose(1, 0, 2)
        layers, batch, slots, heads, head = self_keys.shape
        audios = cross_keys.shape[1]
        keys, vals, ckeys, cvals = flat(self_keys), flat(self_vals), flat(cross_keys), flat(cross_vals)
        prev = None
        for layer in range(layers):
            attn_out, *prev = self_attention(layer, hidden, positions, keys, vals, prev, params)
            hidden = cross_and_mlp(layer, tp, attn_out, hidden, ckeys, cvals, audios, params)

        def unflat(cache):
            return cache.reshape(layers, batch, heads, head, slots).transpose(0, 1, 4, 2, 3)

        return hidden, unflat(prev[0]), unflat(prev[1])

    return jax.shard_map(local_step, mesh=mesh, in_specs=in_specs, out_specs=(P('dp', None), cache_spec, cache_spec), check_vma=False)
```

```python
import functools

import jax
import jax.numpy as jnp
from jax import lax
from jax.experimental import pallas as pl
from jax.experimental.pallas import tpu as pltpu
from jax.sharding import PartitionSpec as P

EPS = 1e-5
NEG = -1e30
PARAM_NAMES = ('ln_gain', 'ln_bias', 'w_query', 'b_query', 'w_key', 'w_value', 'b_value', 'w_out', 'b_out', 'w_cquery', 'b_cquery', 'w_cout', 'b_cout', 'w_fc1', 'b_fc1', 'w_fc2', 'b_fc2')
F32 = jnp.float32
BF16 = jnp.bfloat16
VMEM = pltpu.VMEM
NT = (((1,), (1,)), ((), ()))


def dot(a, b):
    return jnp.dot(a, b, preferred_element_type=F32)


def dot_nt(a, b):
    return lax.dot_general(a, b, NT, preferred_element_type=F32)


def layer_norm(wide_vals, gain_row, bias_row):
    center = wide_vals - jnp.mean(wide_vals, axis=-1, keepdims=True)
    var_est = jnp.mean(center * center, axis=-1, keepdims=True)
    return (center * lax.rsqrt(var_est + EPS) * gain_row + bias_row).astype(BF16)


def iota(shape, dim):
    return lax.broadcasted_iota(jnp.int32, shape, dim)


def stack_eye(rows, width):
    return (iota((width, rows), 1) % width == iota((width, rows), 0)).astype(BF16)


def row(ref, *idx):
    return ref[idx].astype(F32)


def load_all(pairs, sem):
    copies = [pltpu.make_async_copy(src, dst, sem.at[n]) for n, (src, dst) in enumerate(pairs)]
    for copy in copies:
        copy.start()
    return copies


def pack_half(vals):
    half = vals.shape[0] // 2
    return jnp.concatenate([vals[:half], vals[half:]], axis=1).astype(BF16)


def self_kernel(layer, group, streams, fetched, *refs):
    pos_hbm, hidden_in, gain_hbm, bias_hbm, wq_hbm, bq_hbm, wk_hbm, wv_hbm, bv_hbm, kin_ref, vin_ref = refs[:11]
    if fetched:
        o_ref, kout_ref, vout_ref, kbuf, vbuf = refs[13:18]
        hidden_ref = hidden_in
        rest = refs[18:]
    else:
        o_ref, kout_ref, vout_ref, kbuf, vbuf, hidden_ref = refs[11:17]
        rest = refs[17:]
    qbd, kcol, vcol, scores, osc, pos_ref, gain_ref, bias_ref, wq_ref, bq_ref, wk_ref, wv_ref, bv_ref, in_sem, out_sem, param_sem = rest
    batch = hidden_ref.shape[0]
    head = wq_ref.shape[0]
    slots = kbuf.shape[2]
    groups = batch // group
    span = group * head
    base = layer * batch * head
    scale = head ** -0.25

    def in_copy(src, buf, which, g):
        return pltpu.make_async_copy(src.at[pl.ds(base + g * span, span), :], buf.at[g], in_sem.at[which, g])

    def out_copy(buf, dst, which, g):
        return pltpu.make_async_copy(buf.at[g], dst.at[pl.ds(base + g * span, span), :], out_sem.at[which, g])

    pairs = [(gain_hbm, gain_ref), (bias_hbm, bias_ref), (wq_hbm.at[layer], wq_ref), (bq_hbm, bq_ref), (wk_hbm.at[layer], wk_ref), (wv_hbm.at[layer], wv_ref), (bv_hbm, bv_ref), (pos_hbm, pos_ref)]
    if not fetched:
        pairs.append((hidden_in, hidden_ref))
    copies = load_all(pairs, param_sem)

    def start(g, carry):
        in_copy(kin_ref, kbuf, 0, g).start()
        in_copy(vin_ref, vbuf, 1, g).start()
        return carry

    if not fetched:
        lax.fori_loop(0, groups, start, 0)
    for copy in copies:
        copy.wait()

    normed = layer_norm(hidden_ref[...].astype(F32), gain_ref[0, layer:layer + 1, :].astype(F32), bias_ref[0, layer:layer + 1, :].astype(F32))
    q = ((dot_nt(normed, wq_ref[...]) + bq_ref[layer:layer + 1, :].astype(F32)) * scale).astype(BF16)
    k = (dot_nt(normed, wk_ref[...]) * scale).astype(BF16)
    v = (dot_nt(normed, wv_ref[...]) + bv_ref[layer:layer + 1, :].astype(F32)).astype(BF16)
    wide_q = dot(q, stack_eye(span, head))
    diag = iota((batch, span), 0) % group == iota((batch, span), 1) // head
    qbd[...] = jnp.where(diag, wide_q, 0.0)
    k_t = k.astype(F32).T
    v_t = v.astype(F32).T
    for g in range(groups):
        kcol[g] = k_t[:, g * group:(g + 1) * group]
        vcol[g] = v_t[:, g * group:(g + 1) * group]

    full_tiles = slots // 128
    tail = slots - full_tiles * 128

    def rows_of(g, count=1):
        return pl.ds(pl.multiple_of(g * group, group), count * group)

    def update(g):
        if not fetched:
            in_copy(kin_ref, kbuf, 0, g).wait()
            in_copy(vin_ref, vbuf, 1, g).wait()
        kc = kcol[g]
        vc = vcol[g]
        for i in range(group):
            pos = pos_ref[g * group + i]
            rows = slice(i * head, (i + 1) * head)
            first = pl.multiple_of(jnp.minimum(pos // 128, full_tiles - 1) * 128, 128)
            places = [(pl.ds(first, 128), iota((head, 128), 1) + first == pos)]
            if tail:
                places.append((slice(full_tiles * 128, slots), iota((head, tail), 1) + full_tiles * 128 == pos))
            for cols, hit in places:
                for buf, col in ((kbuf, kc), (vbuf, vc)):
                    old = buf[g, rows, cols].astype(F32)
                    buf[g, rows, cols] = jnp.where(hit, col[:, i:i + 1], old).astype(BF16)

    def score(g):
        limit = jnp.zeros((group, 1), jnp.int32)
        for i in range(group):
            limit = jnp.where(iota((group, 1), 0) == i, pos_ref[g * group + i], limit)
        raw = dot(qbd[rows_of(g), :].astype(BF16), kbuf[g])
        scores[rows_of(g), :] = jnp.where(iota((group, slots), 1) <= limit, raw, NEG)

    def weigh(g):
        wide_o = dot_nt(vbuf[g], scores[rows_of(g), :].astype(BF16))
        o_t = jnp.zeros((head, group), F32)
        for i in range(group):
            o_t = o_t + jnp.where(iota((head, group), 1) == i, wide_o[i * head:(i + 1) * head, :], 0.0)
        osc[rows_of(g), :] = o_t.T

    batch_of = 4

    def attend(n, carry):
        first = n * batch_of
        for i in range(batch_of):
            update(first + i)
        for i in range(batch_of):
            score(first + i)
        for i in range(batch_of):
            out_copy(kbuf, kout_ref, 0, first + i).start()
            out_copy(vbuf, vout_ref, 1, first + i).start()
        raw = scores[rows_of(first, batch_of), :]
        probs = jnp.exp(raw - jnp.max(raw, axis=-1, keepdims=True))
        scores[rows_of(first, batch_of), :] = probs * (1.0 / jnp.sum(probs, axis=-1, keepdims=True))
        for i in range(batch_of):
            weigh(first + i)
        return carry

    lax.fori_loop(0, groups // batch_of, attend, 0)
    part = batch // streams
    for s in range(streams):
        o_ref[s] = pack_half(osc[s * part:(s + 1) * part, :])

    def finish(g, carry):
        out_copy(kbuf, kout_ref, 0, g).wait()
        out_copy(vbuf, vout_ref, 1, g).wait()
        return carry

    lax.fori_loop(0, groups, finish, 0)


def in_hbm(arrays):
    return [pltpu.with_memory_space_constraint(a, pltpu.HBM) for a in arrays]


def in_vmem(arrays):
    return [pltpu.with_memory_space_constraint(a, VMEM) for a in arrays]


def self_attention(layer, group, streams, hidden, positions, keys, vals, outs, params):
    fetched = outs is not None
    batch = hidden.shape[0]
    head = params['w_query'].shape[1]
    groups = batch // group
    vm = pl.BlockSpec(memory_space=VMEM)
    hbm = pl.BlockSpec(memory_space=pltpu.HBM)
    small = in_hbm([params[n] for n in ('ln_gain', 'ln_bias', 'w_query', 'b_query', 'w_key', 'w_value', 'b_value')])
    weight = VMEM(params['w_query'].shape[1:], BF16)
    vector = VMEM(params['b_query'].shape, BF16)
    norm = VMEM(params['ln_gain'].shape, BF16)
    if fetched:
        operands = in_hbm([positions]) + in_vmem([hidden]) + small + in_vmem([keys, vals]) + in_hbm(outs)
        in_specs = [hbm, vm] + [hbm] * 7 + [vm] * 2 + [hbm] * 2
        caches = list(outs)
        aliases = {9: 3, 10: 4, 11: 1, 12: 2}
        slots = keys.shape[2]
        extra_out = tuple(VMEM(a.shape, BF16) for a in (keys, vals))
        bufs = []
    else:
        operands = in_hbm([positions, hidden]) + small + in_hbm([keys, vals])
        in_specs = [hbm] * 11
        caches = [keys, vals]
        aliases = {}
        slots = keys.shape[1]
        extra_out = ()
        bufs = [VMEM((groups, group * head, slots), BF16)] * 2 + [VMEM(hidden.shape, BF16)]
    return pl.pallas_call(
        functools.partial(self_kernel, layer, group, streams, fetched),
        out_shape=(jax.ShapeDtypeStruct((streams, batch // streams // 2, 2 * head), BF16),) + tuple(jax.ShapeDtypeStruct(c.shape, BF16) for c in caches) + extra_out,
        in_specs=in_specs,
        out_specs=(vm, hbm, hbm) + (vm,) * len(extra_out),
        scratch_shapes=bufs + [
            VMEM((batch, group * head), F32),
            VMEM((groups, head, group), F32),
            VMEM((groups, head, group), F32),
            VMEM((batch, slots), F32),
            VMEM((batch, head), F32),
            pltpu.SMEM((batch,), jnp.int32),
            norm, norm, weight, vector, weight, weight, vector,
            pltpu.SemaphoreType.DMA((2, groups)),
            pltpu.SemaphoreType.DMA((2, groups)),
            pltpu.SemaphoreType.DMA((9,)),
        ],
        input_output_aliases=aliases,
        compiler_params=pltpu.CompilerParams(vmem_limit_bytes=(12 if fetched else 32) * 2**20),
        name='self_attention',
    )(*operands)[:3]


def cross_kernel(layer, layers, tp, group, streams, *refs):
    first, last = layer == 0, layer + 1 == layers
    refs = list(refs)
    o_ref, hidden_ref = refs[:2]
    param_hbm = refs[2:14]
    kin_ref, vin_ref = refs[14:16]
    del refs[:16]
    wo_in = None if first else refs.pop(0)
    if not last:
        wo_next_hbm, kself_ref, vself_ref = refs[:3]
        del refs[:3]
    hidden_out_ref = refs.pop(0)
    if not last:
        wo_out, kself_out, vself_out = refs[:3]
        del refs[:3]
    param_refs = refs[:12]
    gain_ref, bias_ref, bo_ref, bcq_ref, bco_ref, b1_ref, b2_ref, wo_ref, wcq_ref, wco_ref, w1_ref, w2_ref = param_refs
    (wo_next, kbuf, vbuf, part, landed, blocks, gathered, packed, wide_w, qbd, scores, param_sem, in_sem, self_sem, rs_send, rs_recv, ag_send, ag_recv, g_send, g_recv, w_send, w_recv) = refs[12:]
    me = lax.axis_index('tp')
    batch, width = hidden_ref.shape
    head = wcq_ref.shape[0]
    size = batch // streams
    half = size // 2
    quarters = width // 128
    chunks = kbuf.shape[0]
    span = kbuf.shape[1]
    base = layer * chunks * span
    scale = head ** -0.25
    beams = batch // (chunks * group)
    rows = group * beams
    per_stream = chunks // streams
    peers = [lax.rem(me + step, tp) for step in range(1, tp)]
    same_core = [lax.rem(me + step, tp) for step in range(2, tp, 2)]
    sibling = me + 1 - 2 * lax.rem(me, 2)

    def in_copy(src, buf, which, c):
        return pltpu.make_async_copy(src.at[pl.ds(base + c * span, span), :], buf.at[c], in_sem.at[which, c])

    def remote(src, dst, send_sem, recv_sem, peer):
        return pltpu.make_async_remote_copy(src, dst, send_sem, recv_sem, device_id={'tp': peer}, device_id_type=pl.DeviceIdType.MESH)

    barrier = pltpu.get_barrier_semaphore()
    for peer in peers:
        pl.semaphore_signal(barrier, inc=1, device_id={'tp': peer}, device_id_type=pl.DeviceIdType.MESH)

    pairs = [(src if src.shape == dst.shape else src.at[layer], dst) for src, dst in zip(param_hbm, param_refs)]
    if not last:
        pairs.append((wo_next_hbm.at[layer + 1], wo_next))
    copies = load_all(pairs, param_sem)
    for c in range(chunks):
        in_copy(kin_ref, kbuf, 0, c).start()
        in_copy(vin_ref, vbuf, 1, c).start()
    self_copies = []
    if not last:
        count, rows_self = kself_out.shape[:2]
        start_row = (layer + 1) * count * rows_self

        def self_copy(src, dst, which, g):
            return pltpu.make_async_copy(src.at[pl.ds(start_row + g * rows_self, rows_self), :], dst.at[g], self_sem.at[which, g])

        def start_self(g, carry):
            self_copy(kself_ref, kself_out, 0, g).start()
            self_copy(vself_ref, vself_out, 1, g).start()
            return carry

        def wait_self(g, carry):
            self_copy(kself_ref, kself_out, 0, g).wait()
            self_copy(vself_ref, vself_out, 1, g).wait()
            return carry

        lax.fori_loop(0, count, start_self, 0)
    for copy in copies:
        copy.wait()

    sends = []

    def send(*args):
        copy = remote(*args)
        copy.start()
        sends.append(copy)

    def vec(ref):
        return ref[layer:layer + 1, :].astype(F32)

    def norm(x, k):
        return layer_norm(x, gain_ref[k, layer:layer + 1, :].astype(F32), bias_ref[k, layer:layer + 1, :].astype(F32))

    def bounds(j):
        r, c = j // quarters, j % quarters
        return slice(r * half, (r + 1) * half), slice(c * 128, (c + 1) * 128)

    def scatter(x, s, total, hidden):
        for j in range(tp):
            rs, cs = bounds(j)
            part[x, s, j] = total[rs, cs].astype(BF16)
            blocks[x, s, j] = hidden[rs, cs].astype(BF16)
        for n, peer in enumerate(peers):
            send(part.at[x, s, peer], landed.at[x, s, me], rs_send.at[x, s, n], rs_recv.at[x, s, me], peer)

    def reduce_and_gather(x, s, bias_ref):
        bias = vec(bias_ref)
        own = lax.rem(me, quarters)
        bias_row = jnp.zeros((1, 128), F32)
        for c in range(quarters):
            bias_row = jnp.where(own == c, bias[:, c * 128:(c + 1) * 128], bias_row)
        acc = part[x, s, me].astype(F32) + blocks[x, s, me].astype(F32) + bias_row
        for n, peer in reversed(list(enumerate(peers))):
            remote(part.at[x, s, peer], landed.at[x, s, peer], rs_send.at[x, s, n], rs_recv.at[x, s, peer], peer).wait_recv()
            acc = acc + landed[x, s, peer].astype(F32)
        blocks[x, s, me] = acc.astype(BF16)
        for n, peer in enumerate(peers):
            send(blocks.at[x, s, me], blocks.at[x, s, me], ag_send.at[x, s, n], ag_recv.at[x, s, me], peer)

    def collect(x, s):
        for n, peer in enumerate(peers):
            remote(blocks.at[x, s, peer], blocks.at[x, s, peer], ag_send.at[x, s, n], ag_recv.at[x, s, peer], peer).wait_recv()
        return jnp.concatenate([jnp.concatenate([blocks[x, s, r * quarters + c].astype(F32) for c in range(quarters)], axis=1) for r in range(tp // quarters)], axis=0)

    def share(x, s, src):
        gathered[x, s, me] = src[s]
        for n, peer in enumerate(peers):
            send(src.at[s], gathered.at[x, s, me], g_send.at[x, s, n], g_recv.at[x, s, me], peer)

    def project_all(x, s, w_ref, bias_ref, hidden):
        for n, peer in enumerate(peers):
            remote(gathered.at[x, s, peer], gathered.at[x, s, peer], g_send.at[x, s, n], g_recv.at[x, s, peer], peer).wait_recv()
        vals = [gathered[x, s, j].astype(F32) for j in range(tp)]
        heads = jnp.concatenate([jnp.concatenate([v[:, :head] for v in vals], axis=1), jnp.concatenate([v[:, head:] for v in vals], axis=1)], axis=0)
        whole_w = w_ref[...].reshape(tp * head, width)
        return (hidden + dot(heads.astype(BF16), whole_w) + vec(bias_ref)).astype(BF16).astype(F32)

    def spread_weight(w, src):
        wide_w[w, me] = src[...]
        for n, peer in enumerate(same_core):
            send(src, wide_w.at[w, me], w_send.at[w, n], w_recv.at[w, me], peer)
        send(src, wide_w.at[w, me], w_send.at[w, tp // 2 - 1], w_recv.at[w, me], sibling)

    def forward_weight(w):
        for n, peer in enumerate(same_core):
            remote(wide_w.at[w, peer], wide_w.at[w, peer], w_send.at[w, n], w_recv.at[w, peer], peer).wait_recv()
            send(wide_w.at[w, peer], wide_w.at[w, peer], w_send.at[w, tp // 2 + n], w_recv.at[w, peer], sibling)

    def finish_weight(w):
        for step in range(0, tp, 2):
            origin = lax.rem(sibling + step, tp)
            remote(wide_w.at[w, origin], wide_w.at[w, origin], w_send.at[w, 0], w_recv.at[w, origin], sibling).wait_recv()

    def attend(s, hidden):
        q = ((dot_nt(norm(hidden, 1), wcq_ref[...]) + vec(bcq_ref)) * scale).astype(BF16)
        diag = (iota((size, span), 0) // beams) % group == iota((size, span), 1) // head
        qbd[s] = jnp.where(diag, dot(q, stack_eye(span, head)), 0.0).astype(BF16)
        for c in range(per_stream):
            in_copy(kin_ref, kbuf, 0, s * per_stream + c).wait()
            scores[s, c * rows:(c + 1) * rows, :] = dot(qbd[s, c * rows:(c + 1) * rows, :], kbuf[s * per_stream + c])
        outs = []
        for c in range(per_stream):
            raw = scores[s, c * rows:(c + 1) * rows, :]
            probs = jnp.exp(raw - jnp.max(raw, axis=-1, keepdims=True))
            probs = (probs * (1.0 / jnp.sum(probs, axis=-1, keepdims=True))).astype(BF16)
            in_copy(vin_ref, vbuf, 1, s * per_stream + c).wait()
            wide_o = dot_nt(vbuf[s * per_stream + c], probs)
            o_t = jnp.zeros((head, rows), F32)
            for i in range(group):
                o_t = o_t + jnp.where(iota((head, rows), 1) // beams == i, wide_o[i * head:(i + 1) * head, :], 0.0)
            outs.append(o_t.T)
        packed[s] = pack_half(jnp.concatenate(outs, axis=0))

    def mlp(hidden):
        inner = dot(norm(hidden, 2), w1_ref[...]) + vec(b1_ref)
        return dot((0.5 * inner * (1.0 + lax.erf(inner * (0.5 ** 0.5)))).astype(BF16), w2_ref[...])

    ids = range(streams)
    states = [hidden_ref[s * size:(s + 1) * size, :].astype(F32) for s in ids]
    if first:
        totals = []
        for s in ids:
            mine = o_ref[s].astype(F32)
            mine = jnp.concatenate([mine[:, :head], mine[:, head:]], axis=0).astype(BF16)
            totals.append(dot(mine, wo_ref[...]))
        pl.semaphore_wait(barrier, tp - 1)
        for s in ids:
            scatter(0, s, totals[s], states[s])
        for s in ids:
            reduce_and_gather(0, s, bo_ref)
        spread_weight(0, wco_ref)
        states = [None] * streams
    else:
        pl.semaphore_wait(barrier, tp - 1)
        for s in ids:
            share(0, s, o_ref)
        spread_weight(0, wco_ref)
    for s in ids:
        if first:
            states[s] = collect(0, s)
        else:
            states[s] = project_all(0, s, wo_in, bo_ref, states[s])
        attend(s, states[s])
        share(1, s, packed)
        if s == 0:
            forward_weight(0)
    if not last:
        spread_weight(1, wo_next)
    finish_weight(0)
    for s in ids:
        states[s] = project_all(1, s, wide_w.at[0], bco_ref, states[s])
        scatter(1, s, mlp(states[s]), states[s])
    for s in ids:
        reduce_and_gather(1, s, b2_ref)
    if not last:
        forward_weight(1)
    for s in ids:
        hidden_out_ref[s * size:(s + 1) * size, :] = collect(1, s).astype(BF16)
    if not last:
        finish_weight(1)
        wo_out[...] = wide_w[1]
        lax.fori_loop(0, count, wait_self, 0)
    for copy in sends:
        copy.wait_send()


def cross_and_mlp(layer, layers, tp, group, streams, attn_out, hidden, keys, vals, audios, params, wo_full, selfs, self_group):
    batch, width = hidden.shape
    head = params['w_cquery'].shape[1]
    frames = keys.shape[1]
    chunks = audios // group
    first, last = layer == 0, layer + 1 == layers
    vm = pl.BlockSpec(memory_space=VMEM)
    hbm = pl.BlockSpec(memory_space=pltpu.HBM)
    vectors = ('ln_gain', 'ln_bias', 'b_out', 'b_cquery', 'b_cout', 'b_fc1', 'b_fc2')
    weights = ('w_out', 'w_cquery', 'w_cout', 'w_fc1', 'w_fc2')
    operands = in_vmem([attn_out, hidden]) + in_hbm([params[n] for n in vectors + weights] + [keys, vals])
    in_specs = [vm] * 2 + [hbm] * 14
    out_shape = [VMEM((batch, width), BF16)]
    out_specs = [vm]
    wide = (tp,) + params['w_out'].shape[1:]
    if not first:
        operands += in_vmem([wo_full])
        in_specs += [vm]
    if not last:
        operands += in_hbm([params['w_out'], *selfs])
        in_specs += [hbm] * 3
        cache = (batch // self_group, self_group * head, selfs[0].shape[1])
        out_shape += [VMEM(wide, BF16), VMEM(cache, BF16), VMEM(cache, BF16)]
        out_specs += [vm] * 3
    block = (batch // streams // 2, 128)
    dma = pltpu.SemaphoreType.DMA
    return pl.pallas_call(
        functools.partial(cross_kernel, layer, layers, tp, group, streams),
        out_shape=tuple(out_shape),
        in_specs=in_specs,
        out_specs=tuple(out_specs),
        scratch_shapes=[VMEM(params[n].shape, BF16) for n in vectors] + [VMEM(params[n].shape[1:], BF16) for n in weights] + [
            VMEM(params['w_out'].shape[1:], BF16),
            VMEM((chunks, group * head, frames), BF16),
            VMEM((chunks, group * head, frames), BF16),
            VMEM((2, streams, tp) + block, BF16),
            VMEM((2, streams, tp) + block, BF16),
            VMEM((2, streams, tp) + block, BF16),
            VMEM((2, streams, tp) + block, BF16),
            VMEM((streams,) + block, BF16),
            VMEM((2,) + wide, BF16),
            VMEM((streams, batch // streams, group * head), BF16),
            VMEM((streams, batch // streams, frames), F32),
            dma((13,)),
            dma((2, chunks)),
            dma((2, batch // self_group)),
            dma((2, streams, tp - 1)),
            dma((2, streams, tp)),
            dma((2, streams, tp - 1)),
            dma((2, streams, tp)),
            dma((2, streams, tp - 1)),
            dma((2, streams, tp)),
            dma((2, tp)),
            dma((2, tp)),
        ],
        compiler_params=pltpu.CompilerParams(vmem_limit_bytes=24 * 2**20, collective_id=layer, has_side_effects=True),
        name='cross_and_mlp',
    )(*operands)


def solution(mesh):
    tp = mesh.shape['tp']
    cache_spec = P(None, 'dp', None, 'tp', None)
    col_spec = P(None, None, 'tp')
    row_spec = P(None, 'tp', None)
    vec_spec = P(None, 'tp')
    param_specs = {'ln_gain': P(), 'ln_bias': P(), 'w_query': col_spec, 'b_query': vec_spec, 'w_key': col_spec, 'w_value': col_spec, 'b_value': vec_spec, 'w_out': row_spec, 'b_out': P(), 'w_cquery': col_spec, 'b_cquery': vec_spec, 'w_cout': row_spec, 'b_cout': P(), 'w_fc1': col_spec, 'b_fc1': vec_spec, 'w_fc2': row_spec, 'b_fc2': P()}
    in_specs = (P('dp', None), P('dp'), cache_spec, cache_spec, cache_spec, cache_spec) + tuple(param_specs[param_name] for param_name in PARAM_NAMES)

    def flat(cache):
        layers, n, slots, heads, head = cache.shape
        return cache.transpose(0, 1, 3, 4, 2).reshape(layers * n * heads * head, slots)

    def local_step(hidden, positions, self_keys, self_vals, cross_keys, cross_vals, *layer_params):
        params = dict(zip(PARAM_NAMES, layer_params))
        for name in ('w_query', 'w_key', 'w_value', 'w_cquery'):
            params[name] = params[name].transpose(0, 2, 1)
        for name in ('ln_gain', 'ln_bias'):
            params[name] = params[name].transpose(1, 0, 2)
        layers, batch, slots, heads, head = self_keys.shape
        audios = cross_keys.shape[1]
        keys, vals, ckeys, cvals = flat(self_keys), flat(self_vals), flat(cross_keys), flat(cross_vals)
        streams, group, cross_group = 2, 8, 8
        outs, wo_full, keys_now, vals_now = None, None, keys, vals
        for layer in range(layers):
            attn_out, *outs = self_attention(layer, group, streams, hidden, positions, keys_now, vals_now, outs, params)
            hidden, *rest = cross_and_mlp(layer, layers, tp, cross_group, streams, attn_out, hidden, ckeys, cvals, audios, params, wo_full, (keys, vals), group)
            if rest:
                wo_full, keys_now, vals_now = rest

        def unflat(cache):
            return cache.reshape(layers, batch, heads, head, slots).transpose(0, 1, 4, 2, 3)

        return hidden, unflat(outs[0]), unflat(outs[1])

    return jax.shard_map(local_step, mesh=mesh, in_specs=in_specs, out_specs=(P('dp', None), cache_spec, cache_spec), check_vma=False)
```

```python
import functools

import jax
import jax.numpy as jnp
from jax import lax
from jax.experimental import pallas as pl
from jax.experimental.pallas import tpu as pltpu
from jax.sharding import PartitionSpec as P

EPS = 1e-5
NEG = -1e30
PARAM_NAMES = ('ln_gain', 'ln_bias', 'w_query', 'b_query', 'w_key', 'w_value', 'b_value', 'w_out', 'b_out', 'w_cquery', 'b_cquery', 'w_cout', 'b_cout', 'w_fc1', 'b_fc1', 'w_fc2', 'b_fc2')
F32 = jnp.float32
BF16 = jnp.bfloat16
VMEM = pltpu.VMEM
NT = (((1,), (1,)), ((), ()))


def dot(a, b):
    return jnp.dot(a, b, preferred_element_type=F32)


def dot_nt(a, b):
    return lax.dot_general(a, b, NT, preferred_element_type=F32)


def layer_norm(wide_vals, gain_row, bias_row):
    center = wide_vals - jnp.mean(wide_vals, axis=-1, keepdims=True)
    var_est = jnp.mean(center * center, axis=-1, keepdims=True)
    return (center * lax.rsqrt(var_est + EPS) * gain_row + bias_row).astype(BF16)


def repeat_lanes(vals, width):
    pair = jnp.concatenate([vals, vals], axis=1)
    return jnp.concatenate([pair] * (width // pair.shape[1]), axis=1)


def iota(shape, dim):
    return lax.broadcasted_iota(jnp.int32, shape, dim)


def load_all(pairs, sem):
    copies = [pltpu.make_async_copy(src, dst, sem.at[n]) for n, (src, dst) in enumerate(pairs)]
    for copy in copies:
        copy.start()
    return copies


def pack_half(vals):
    half = vals.shape[0] // 2
    return jnp.concatenate([vals[:half], vals[half:]], axis=1).astype(BF16)


def pack_half(vals):
    half = vals.shape[0] // 2
    return jnp.concatenate([vals[:half], vals[half:]], axis=1).astype(BF16)


def in_hbm(arrays):
    return [pltpu.with_memory_space_constraint(a, pltpu.HBM) for a in arrays]


def in_vmem(arrays):
    return [pltpu.with_memory_space_constraint(a, VMEM) for a in arrays]


VECTORS = ('ln_gain', 'ln_bias', 'b_query', 'b_value', 'b_out', 'b_cquery', 'b_cout', 'b_fc1', 'b_fc2')
WEIGHTS = ('w_query', 'w_key', 'w_value', 'w_out', 'w_cquery', 'w_cout', 'w_fc1', 'w_fc2')


def write_kernel(group, layers, pos_hbm, hidden_ref, knew_ref, vnew_ref, *refs):
    hidden_out_ref, kout_ref, vout_ref = refs[2 * layers:2 * layers + 3]
    kbufs = refs[2 * layers + 3:3 * layers + 3]
    vbufs = refs[3 * layers + 3:4 * layers + 3]
    kcol, vcol, pos_ref, pos_sem, hidden_sem, out_sem = refs[4 * layers + 3:]
    batch, head = knew_ref.shape[1:]
    groups, span, slots = kbufs[0].shape
    pos_copy = pltpu.make_async_copy(pos_hbm, pos_ref, pos_sem)
    pos_copy.start()
    hidden_copy = pltpu.make_async_copy(hidden_ref, hidden_out_ref, hidden_sem)
    hidden_copy.start()

    def out_copy(layer, which, g):
        buf, dst = ((kbufs[layer], kout_ref), (vbufs[layer], vout_ref))[which]
        return pltpu.make_async_copy(buf.at[g], dst.at[pl.ds((layer * groups + g) * span, span), :], out_sem.at[layer, which, g])

    full_tiles = slots // 128
    tail = slots - full_tiles * 128
    for layer in range(layers):
        k_t = knew_ref[layer].astype(F32).T
        v_t = vnew_ref[layer].astype(F32).T
        for g in range(groups):
            kcol[layer, g] = k_t[:, g * group:(g + 1) * group]
            vcol[layer, g] = v_t[:, g * group:(g + 1) * group]
    pos_copy.wait()

    for layer in range(layers):
        def update(g, carry):
            cols_of = (kcol[layer, g], vcol[layer, g])
            for i in range(group):
                pos = pos_ref[g * group + i]
                rows = slice(i * head, (i + 1) * head)
                first = pl.multiple_of(jnp.minimum(pos // 128, full_tiles - 1) * 128, 128)
                places = [(pl.ds(first, 128), iota((head, 128), 1) + first == pos)]
                if tail:
                    places.append((slice(full_tiles * 128, slots), iota((head, tail), 1) + full_tiles * 128 == pos))
                for cols, hit in places:
                    for buf, col in zip((kbufs[layer], vbufs[layer]), cols_of):
                        old = buf[g, rows, cols].astype(F32)
                        buf[g, rows, cols] = jnp.where(hit, col[:, i:i + 1], old).astype(BF16)
            out_copy(layer, 0, g).start()
            out_copy(layer, 1, g).start()
            return carry

        lax.fori_loop(0, groups, update, 0)

    for layer in range(layers):
        def finish(g, carry):
            out_copy(layer, 0, g).wait()
            out_copy(layer, 1, g).wait()
            return carry

        lax.fori_loop(0, groups, finish, 0)
    hidden_copy.wait()


def write_caches(group, positions, hidden, knew, vnew, kbufs, vbufs, flat_shape):
    layers, batch, head = knew.shape
    groups = kbufs[0].shape[0]
    vm = pl.BlockSpec(memory_space=VMEM)
    hbm = pl.BlockSpec(memory_space=pltpu.HBM)
    caches = list(kbufs) + list(vbufs)
    dma = pltpu.SemaphoreType.DMA
    return pl.pallas_call(
        functools.partial(write_kernel, group, layers),
        out_shape=(jax.ShapeDtypeStruct(hidden.shape, BF16),) + (jax.ShapeDtypeStruct(flat_shape, BF16),) * 2 + tuple(VMEM(c.shape, BF16) for c in caches),
        in_specs=[hbm] + [vm] * (3 + len(caches)),
        out_specs=(hbm, hbm, hbm) + (vm,) * len(caches),
        scratch_shapes=[
            VMEM((layers, groups, head, group), F32),
            VMEM((layers, groups, head, group), F32),
            pltpu.SMEM((batch,), jnp.int32),
            dma,
            dma,
            dma((layers, 2, groups)),
        ],
        input_output_aliases={4 + n: 3 + n for n in range(len(caches))},
        compiler_params=pltpu.CompilerParams(vmem_limit_bytes=43 * 2**19),
        name='write_caches',
    )(*in_hbm([positions]), *in_vmem([hidden, knew, vnew] + caches))[:3]


def layers_kernel(layers, tp, group, cross_group, streams, *refs):
    refs = list(refs)
    counts = (2, len(VECTORS), len(WEIGHTS), 4, 3, layers, layers, 2, len(VECTORS), len(WEIGHTS))
    split = []
    for count in counts:
        split.append(refs[:count])
        del refs[:count]
    (pos_hbm, hidden_hbm), vec_hbm, weight_hbm, (kself_ref, vself_ref, kin_ref, vin_ref), (hidden_out_ref, knew_ref, vnew_ref), kselfs, vselfs, (pos_ref, hidden_ref), vec_refs, weight_refs = split
    gain_ref, bias_ref, bq_ref, bv_ref, bo_ref, bcq_ref, bco_ref, b1_ref, b2_ref = vec_refs
    wq_ref, wk_ref, wv_ref, wo_ref, wcq_ref, wco_ref, w1_ref, w2_ref = weight_refs
    (kbuf, vbuf, part, landed, blocks, gathered, packed, wide_w, qself, sself, oself, qbd, scores, param_sem, self_sem, in_sem, rs_send, rs_recv, ag_send, ag_recv, g_send, g_recv, w_send, w_recv) = refs
    me = lax.axis_index('tp')
    batch, width = hidden_ref.shape
    head = wcq_ref.shape[1]
    size = batch // streams
    half = size // 2
    quarters = width // 128
    scale = head ** -0.25
    groups, span, slots = kselfs[0].shape
    chunks, cross_span = kbuf.shape[:2]
    beams = batch // (chunks * cross_group)
    rows = cross_group * beams
    per_stream = chunks // streams
    peers = [lax.rem(me + step, tp) for step in range(1, tp)]
    same_core = [lax.rem(me + step, tp) for step in range(2, tp, 2)]
    sibling = me + 1 - 2 * lax.rem(me, 2)
    ids = range(streams)

    def remote(src, dst, send_sem, recv_sem, peer):
        return pltpu.make_async_remote_copy(src, dst, send_sem, recv_sem, device_id={'tp': peer}, device_id_type=pl.DeviceIdType.MESH)

    barrier = pltpu.get_barrier_semaphore()
    for peer in peers:
        pl.semaphore_signal(barrier, inc=1, device_id={'tp': peer}, device_id_type=pl.DeviceIdType.MESH)

    copies = load_all(list(zip([pos_hbm, hidden_hbm] + vec_hbm + weight_hbm, [pos_ref, hidden_ref] + vec_refs + weight_refs)), param_sem)

    def self_copy(layer, which, g):
        src, dst = ((kself_ref, kselfs[layer]), (vself_ref, vselfs[layer]))[which]
        return pltpu.make_async_copy(src.at[pl.ds((layer * groups + g) * span, span), :], dst.at[g], self_sem.at[layer, which, g])

    def start_self(layer):
        def start(g, carry):
            self_copy(layer, 0, g).start()
            self_copy(layer, 1, g).start()
            return carry

        lax.fori_loop(0, groups, start, 0)

    def cross_copy(layer, which, c):
        src, buf = ((kin_ref, kbuf), (vin_ref, vbuf))[which]
        return pltpu.make_async_copy(src.at[pl.ds((layer * chunks + c) * cross_span, cross_span), :], buf.at[c], in_sem.at[layer, which, c])

    start_self(0)
    for copy in copies:
        copy.wait()
    sends = []

    def send(*args):
        copy = remote(*args)
        copy.start()
        sends.append(copy)

    def vec(ref, layer):
        return ref[layer:layer + 1, :].astype(F32)

    def norm(x, layer, k):
        return layer_norm(x, gain_ref[k, layer:layer + 1, :].astype(F32), bias_ref[k, layer:layer + 1, :].astype(F32))

    def bounds(j):
        r, c = j // quarters, j % quarters
        return slice(r * half, (r + 1) * half), slice(c * 128, (c + 1) * 128)

    def scatter(x, s, total, hidden):
        for j in range(tp):
            rs, cs = bounds(j)
            part[x, s, j] = total[rs, cs].astype(BF16)
            blocks[x, s, j] = hidden[rs, cs].astype(BF16)
        for n, peer in enumerate(peers):
            send(part.at[x, s, peer], landed.at[x, s, me], rs_send.at[x, s, n], rs_recv.at[x, s, me], peer)

    def reduce_and_gather(x, s, bias):
        own = lax.rem(me, quarters)
        bias_row = jnp.zeros((1, 128), F32)
        for c in range(quarters):
            bias_row = jnp.where(own == c, bias[:, c * 128:(c + 1) * 128], bias_row)
        for n, peer in reversed(list(enumerate(peers))):
            remote(part.at[x, s, peer], landed.at[x, s, peer], rs_send.at[x, s, n], rs_recv.at[x, s, peer], peer).wait_recv()
        acc = part[x, s, me].astype(F32) + blocks[x, s, me].astype(F32) + bias_row
        for peer in peers:
            acc = acc + landed[x, s, peer].astype(F32)
        blocks[x, s, me] = acc.astype(BF16)
        for n, peer in enumerate(peers):
            send(blocks.at[x, s, me], blocks.at[x, s, me], ag_send.at[x, s, n], ag_recv.at[x, s, me], peer)

    def collect(x, s):
        for n, peer in enumerate(peers):
            remote(blocks.at[x, s, peer], blocks.at[x, s, peer], ag_send.at[x, s, n], ag_recv.at[x, s, peer], peer).wait_recv()
        return jnp.concatenate([jnp.concatenate([blocks[x, s, r * quarters + c].astype(F32) for c in range(quarters)], axis=1) for r in range(tp // quarters)], axis=0)

    def share(x, s, vals):
        packed[x, s] = pack_half(vals)
        gathered[x, s, me] = packed[x, s]
        for n, peer in enumerate(peers):
            send(packed.at[x, s], gathered.at[x, s, me], g_send.at[x, s, n], g_recv.at[x, s, me], peer)

    def project_all(x, s, bias, hidden):
        for n, peer in enumerate(peers):
            remote(packed.at[x, s], gathered.at[x, s, peer], g_send.at[x, s, n], g_recv.at[x, s, peer], peer).wait_recv()
        vals = [gathered[x, s, j].astype(F32) for j in range(tp)]
        heads = jnp.concatenate([jnp.concatenate([v[:, :head] for v in vals], axis=1), jnp.concatenate([v[:, head:] for v in vals], axis=1)], axis=0)
        return (hidden + dot(heads.astype(BF16), wide_w[x].reshape(tp * head, width)) + bias).astype(BF16).astype(F32)

    def spread_weight(x):
        src = (wo_ref, wco_ref)[x % 2].at[x // 2]
        wide_w[x, me] = (wo_ref, wco_ref)[x % 2][x // 2]
        for n, peer in enumerate(same_core):
            send(src, wide_w.at[x, me], w_send.at[x, n], w_recv.at[x, me], peer)
        send(src, wide_w.at[x, me], w_send.at[x, tp // 2 - 1], w_recv.at[x, me], sibling)

    def forward_weight(x):
        for n, peer in enumerate(same_core):
            remote(wide_w.at[x, peer], wide_w.at[x, peer], w_send.at[x, n], w_recv.at[x, peer], peer).wait_recv()
            send(wide_w.at[x, peer], wide_w.at[x, peer], w_send.at[x, tp // 2 + n], w_recv.at[x, peer], sibling)

    def finish_weight(x):
        for step in range(0, tp, 2):
            origin = lax.rem(sibling + step, tp)
            remote(wide_w.at[x, origin], wide_w.at[x, origin], w_send.at[x, 0], w_recv.at[x, origin], sibling).wait_recv()

    self_batch = 5

    def self_attend(layer, s, hidden, after_projections):
        normed = norm(hidden, layer, 0)
        q = ((dot_nt(normed, wq_ref[layer]) + vec(bq_ref, layer)) * scale).astype(BF16)
        k = (dot_nt(normed, wk_ref[layer]) * scale).astype(BF16)
        v = (dot_nt(normed, wv_ref[layer]) + vec(bv_ref, layer)).astype(BF16)
        mine = slice(s * size, (s + 1) * size)
        knew_ref[layer, mine, :] = k
        vnew_ref[layer, mine, :] = v
        diag = iota((size, span), 0) % group == iota((size, span), 1) // head
        qself[...] = jnp.where(diag, repeat_lanes(q.astype(F32), span), 0.0)
        new_score = jnp.sum(q.astype(F32) * k.astype(F32), axis=-1, keepdims=True)
        after_projections()
        first_group = s * (size // group)

        count = size // group

        def score(g):
            limit = jnp.zeros((group, 1), jnp.int32)
            for i in range(group):
                limit = jnp.where(iota((group, 1), 0) == i, pos_ref[(first_group + g) * group + i], limit)
            raw = dot(qself[g * group:(g + 1) * group, :].astype(BF16), kselfs[layer][first_group + g])
            sself[g * group:(g + 1) * group, :] = jnp.where(iota((group, slots), 1) < limit, raw, NEG)

        def weigh(g):
            wide_o = dot_nt(vselfs[layer][first_group + g], sself[g * group:(g + 1) * group, :].astype(BF16))
            o_t = jnp.zeros((head, group), F32)
            for i in range(group):
                o_t = o_t + jnp.where(iota((head, group), 1) == i, wide_o[i * head:(i + 1) * head, :], 0.0)
            oself[g * group:(g + 1) * group, :] = o_t.T

        def batched(step, which):
            for n in range(0, count, self_batch):
                for g in range(n, n + self_batch):
                    self_copy(layer, which, first_group + g).wait()
                for g in range(n, n + self_batch):
                    step(g)

        batched(score, 0)
        raw = sself[...]
        top = jnp.maximum(jnp.max(raw, axis=-1, keepdims=True), new_score)
        probs = jnp.exp(raw - top)
        new_prob = jnp.exp(new_score - top)
        inv = 1.0 / (jnp.sum(probs, axis=-1, keepdims=True) + new_prob)
        sself[...] = probs * inv
        batched(weigh, 1)
        return oself[...] + (new_prob * inv).astype(BF16).astype(F32) * v.astype(F32)

    def cross_attend(layer, s, hidden):
        q = ((dot_nt(norm(hidden, layer, 1), wcq_ref[layer]) + vec(bcq_ref, layer)) * scale).astype(BF16)
        diag = (iota((size, cross_span), 0) // beams) % cross_group == iota((size, cross_span), 1) // head
        qbd[s] = jnp.where(diag, repeat_lanes(q.astype(F32), cross_span), 0.0).astype(BF16)
        for c in range(per_stream):
            cross_copy(layer, 0, s * per_stream + c).wait()
            cross_copy(layer, 1, s * per_stream + c).wait()
        for c in range(per_stream):
            scores[s, c * rows:(c + 1) * rows, :] = dot(qbd[s, c * rows:(c + 1) * rows, :], kbuf[s * per_stream + c])
        outs = []
        for c in range(per_stream):
            raw = scores[s, c * rows:(c + 1) * rows, :]
            probs = jnp.exp(raw - jnp.max(raw, axis=-1, keepdims=True))
            probs = (probs * (1.0 / jnp.sum(probs, axis=-1, keepdims=True))).astype(BF16)
            wide_o = dot_nt(vbuf[s * per_stream + c], probs)
            o_t = jnp.zeros((head, rows), F32)
            for i in range(cross_group):
                o_t = o_t + jnp.where(iota((head, rows), 1) // beams == i, wide_o[i * head:(i + 1) * head, :], 0.0)
            outs.append(o_t.T)
        return jnp.concatenate(outs, axis=0)

    def start_cross(layer, s):
        for c in range(s * per_stream, (s + 1) * per_stream):
            cross_copy(layer, 0, c).start()
            cross_copy(layer, 1, c).start()

    def mlp(layer, hidden):
        inner = dot(norm(hidden, layer, 2), w1_ref[layer]) + vec(b1_ref, layer)
        return dot((0.5 * inner * (1.0 + lax.erf(inner * (0.5 ** 0.5)))).astype(BF16), w2_ref[layer])

    def enter():
        pl.semaphore_wait(barrier, tp - 1)
        spread_weight(0)

    states = [hidden_ref[s * size:(s + 1) * size, :].astype(F32) for s in ids]
    for layer in range(layers):
        early, late = 2 * layer, 2 * layer + 1
        for s in ids:
            if layer:
                states[s] = collect(layer - 1, s)
            begin = layer == 0 and s == 0
            share(early, s, self_attend(layer, s, states[s], enter if begin else lambda: None))
            if layer == 0:
                start_cross(0, s)
        if layer == 0:
            spread_weight(late)
            forward_weight(early)
        if layer + 1 < layers:
            start_self(layer + 1)
        finish_weight(early)
        for s in ids:
            states[s] = project_all(early, s, vec(bo_ref, layer), states[s])
            share(late, s, cross_attend(layer, s, states[s]))
            if layer + 1 < layers:
                start_cross(layer + 1, s)
            if s == 0 and layer == 0:
                forward_weight(late)
        finish_weight(late)
        if layer + 1 < layers:
            spread_weight(early + 2)
            spread_weight(late + 2)
        for s in ids:
            states[s] = project_all(late, s, vec(bco_ref, layer), states[s])
            scatter(layer, s, mlp(layer, states[s]), states[s])
        for s in ids:
            reduce_and_gather(layer, s, vec(b2_ref, layer))
        if layer + 1 < layers:
            forward_weight(early + 2)
            forward_weight(late + 2)
    for s in ids:
        hidden_out_ref[s * size:(s + 1) * size, :] = collect(layers - 1, s).astype(BF16)
    for copy in sends:
        copy.wait_send()


def run_layers(tp, group, cross_group, streams, hidden, positions, keys, vals, ckeys, cvals, params):
    batch, width = hidden.shape
    layers, head = params['w_cquery'].shape[:2]
    slots, frames = keys.shape[1], ckeys.shape[1]
    chunks = ckeys.shape[0] // layers // head // cross_group
    groups = batch // group
    size = batch // streams
    vm = pl.BlockSpec(memory_space=VMEM)
    hbm = pl.BlockSpec(memory_space=pltpu.HBM)
    operands = [positions, hidden] + [params[n] for n in VECTORS + WEIGHTS] + [keys, vals, ckeys, cvals]
    cache = VMEM((groups, group * head, slots), BF16)
    fresh = VMEM((layers, batch, head), BF16)
    block = (size // 2, 128)
    dma = pltpu.SemaphoreType.DMA
    hidden_out, knew, vnew, *caches = pl.pallas_call(
        functools.partial(layers_kernel, layers, tp, group, cross_group, streams),
        out_shape=(VMEM(hidden.shape, BF16), fresh, fresh) + (cache,) * (2 * layers),
        in_specs=[hbm] * len(operands),
        out_specs=(vm,) * (3 + 2 * layers),
        scratch_shapes=[pltpu.SMEM((batch,), jnp.int32), VMEM(hidden.shape, BF16)] + [VMEM(params[n].shape, BF16) for n in VECTORS + WEIGHTS] + [
            VMEM((chunks, cross_group * head, frames), BF16),
            VMEM((chunks, cross_group * head, frames), BF16),
            VMEM((layers, streams, tp) + block, BF16),
            VMEM((layers, streams, tp) + block, BF16),
            VMEM((layers, streams, tp) + block, BF16),
            VMEM((2 * layers, streams, tp) + block, BF16),
            VMEM((2 * layers, streams) + block, BF16),
            VMEM((2 * layers, tp) + params['w_out'].shape[1:], BF16),
            VMEM((size, group * head), F32),
            VMEM((size, slots), F32),
            VMEM((size, head), F32),
            VMEM((streams, size, cross_group * head), BF16),
            VMEM((streams, size, frames), F32),
            dma((2 + len(VECTORS) + len(WEIGHTS),)),
            dma((layers, 2, groups)),
            dma((layers, 2, chunks)),
            dma((layers, streams, tp - 1)),
            dma((layers, streams, tp)),
            dma((layers, streams, tp - 1)),
            dma((layers, streams, tp)),
            dma((2 * layers, streams, tp - 1)),
            dma((2 * layers, streams, tp)),
            dma((2 * layers, tp)),
            dma((2 * layers, tp)),
        ],
        compiler_params=pltpu.CompilerParams(vmem_limit_bytes=43 * 2**19, collective_id=0, has_side_effects=True),
        name='decoder_layers',
    )(*in_hbm(operands))
    return hidden_out, knew, vnew, caches[:layers], caches[layers:]


def solution(mesh):
    tp = mesh.shape['tp']
    cache_spec = P(None, 'dp', None, 'tp', None)
    col_spec = P(None, None, 'tp')
    row_spec = P(None, 'tp', None)
    vec_spec = P(None, 'tp')
    param_specs = {'ln_gain': P(), 'ln_bias': P(), 'w_query': col_spec, 'b_query': vec_spec, 'w_key': col_spec, 'w_value': col_spec, 'b_value': vec_spec, 'w_out': row_spec, 'b_out': P(), 'w_cquery': col_spec, 'b_cquery': vec_spec, 'w_cout': row_spec, 'b_cout': P(), 'w_fc1': col_spec, 'b_fc1': vec_spec, 'w_fc2': row_spec, 'b_fc2': P()}
    in_specs = (P('dp', None), P('dp'), cache_spec, cache_spec, cache_spec, cache_spec) + tuple(param_specs[param_name] for param_name in PARAM_NAMES)

    def flat(cache):
        layers, n, slots, heads, head = cache.shape
        return cache.transpose(0, 1, 3, 4, 2).reshape(layers * n * heads * head, slots)

    def local_step(hidden, positions, self_keys, self_vals, cross_keys, cross_vals, *layer_params):
        params = dict(zip(PARAM_NAMES, layer_params))
        for name in ('w_query', 'w_key', 'w_value', 'w_cquery'):
            params[name] = params[name].transpose(0, 2, 1)
        for name in ('ln_gain', 'ln_bias'):
            params[name] = params[name].transpose(1, 0, 2)
        layers, batch, slots, heads, head = self_keys.shape
        keys, vals, ckeys, cvals = flat(self_keys), flat(self_vals), flat(cross_keys), flat(cross_vals)
        streams, group, cross_group = 2, 8, 8
        hidden, knew, vnew, kbufs, vbufs = run_layers(tp, group, cross_group, streams, hidden, positions, keys, vals, ckeys, cvals, params)
        hidden, *outs = write_caches(group, positions, hidden, knew, vnew, kbufs, vbufs, keys.shape)

        def unflat(cache):
            return cache.reshape(layers, batch, heads, head, slots).transpose(0, 1, 4, 2, 3)

        return hidden, unflat(outs[0]), unflat(outs[1])

    return jax.shard_map(local_step, mesh=mesh, in_specs=in_specs, out_specs=(P('dp', None), cache_spec, cache_spec), check_vma=False)
```

```python
import functools

import jax
import jax.numpy as jnp
from jax import lax
from jax.experimental import pallas as pl
from jax.experimental.pallas import tpu as pltpu
from jax.sharding import PartitionSpec as P

EPS = 1e-5
NEG = -1e30
PARAM_NAMES = ('ln_gain', 'ln_bias', 'w_query', 'b_query', 'w_key', 'w_value', 'b_value', 'w_out', 'b_out', 'w_cquery', 'b_cquery', 'w_cout', 'b_cout', 'w_fc1', 'b_fc1', 'w_fc2', 'b_fc2')
F32 = jnp.float32
BF16 = jnp.bfloat16
VMEM = pltpu.VMEM
NT = (((1,), (1,)), ((), ()))


def dot(a, b):
    return jnp.dot(a, b, preferred_element_type=F32)


def dot_nt(a, b):
    return lax.dot_general(a, b, NT, preferred_element_type=F32)


def layer_norm(wide_vals, gain_row, bias_row):
    center = wide_vals - jnp.mean(wide_vals, axis=-1, keepdims=True)
    var_est = jnp.mean(center * center, axis=-1, keepdims=True)
    return (center * lax.rsqrt(var_est + EPS) * gain_row + bias_row).astype(BF16)


def repeat_lanes(vals, width):
    pair = jnp.concatenate([vals, vals], axis=1)
    return jnp.concatenate([pair] * (width // pair.shape[1]), axis=1)


def iota(shape, dim):
    return lax.broadcasted_iota(jnp.int32, shape, dim)


def load_all(pairs, sem):
    copies = [pltpu.make_async_copy(src, dst, sem.at[n]) for n, (src, dst) in enumerate(pairs)]
    for copy in copies:
        copy.start()
    return copies


def pack_half(vals):
    half = vals.shape[0] // 2
    return jnp.concatenate([vals[:half], vals[half:]], axis=1).astype(BF16)


def pack_half(vals):
    half = vals.shape[0] // 2
    return jnp.concatenate([vals[:half], vals[half:]], axis=1).astype(BF16)


def in_hbm(arrays):
    return [pltpu.with_memory_space_constraint(a, pltpu.HBM) for a in arrays]


def in_vmem(arrays):
    return [pltpu.with_memory_space_constraint(a, VMEM) for a in arrays]


VECTORS = ('ln_gain', 'ln_bias', 'b_query', 'b_value', 'b_out', 'b_cquery', 'b_cout', 'b_fc1', 'b_fc2')
WEIGHTS = ('w_query', 'w_key', 'w_value', 'w_out', 'w_cquery', 'w_cout', 'w_fc1', 'w_fc2')


def write_kernel(group, layers, pos_hbm, hidden_ref, knew_ref, vnew_ref, *refs):
    hidden_out_ref, kout_ref, vout_ref = refs[2 * layers:2 * layers + 3]
    kbufs = refs[2 * layers + 3:3 * layers + 3]
    vbufs = refs[3 * layers + 3:4 * layers + 3]
    kcol, vcol, pos_ref, pos_sem, hidden_sem, out_sem = refs[4 * layers + 3:]
    batch, head = knew_ref.shape[1:]
    groups, span, slots = kbufs[0].shape
    pos_copy = pltpu.make_async_copy(pos_hbm, pos_ref, pos_sem)
    pos_copy.start()
    hidden_copy = pltpu.make_async_copy(hidden_ref, hidden_out_ref, hidden_sem)
    hidden_copy.start()

    def out_copy(layer, which, g):
        buf, dst = ((kbufs[layer], kout_ref), (vbufs[layer], vout_ref))[which]
        return pltpu.make_async_copy(buf.at[g], dst.at[pl.ds((layer * groups + g) * span, span), :], out_sem.at[layer, which, g])

    full_tiles = slots // 128
    tail = slots - full_tiles * 128
    for layer in range(layers):
        k_t = knew_ref[layer].astype(F32).T
        v_t = vnew_ref[layer].astype(F32).T
        for g in range(groups):
            kcol[layer, g] = k_t[:, g * group:(g + 1) * group]
            vcol[layer, g] = v_t[:, g * group:(g + 1) * group]
        if layer == 0:
            pos_copy.wait()

        def update(g, carry):
            cols_of = (kcol[layer, g], vcol[layer, g])
            for i in range(group):
                pos = pos_ref[g * group + i]
                rows = slice(i * head, (i + 1) * head)
                first = pl.multiple_of(jnp.minimum(pos // 128, full_tiles - 1) * 128, 128)
                places = [(pl.ds(first, 128), iota((head, 128), 1) + first == pos)]
                if tail:
                    places.append((slice(full_tiles * 128, slots), iota((head, tail), 1) + full_tiles * 128 == pos))
                for cols, hit in places:
                    for buf, col in zip((kbufs[layer], vbufs[layer]), cols_of):
                        old = buf[g, rows, cols].astype(F32)
                        buf[g, rows, cols] = jnp.where(hit, col[:, i:i + 1], old).astype(BF16)
            out_copy(layer, 0, g).start()
            out_copy(layer, 1, g).start()
            return carry

        lax.fori_loop(0, groups, update, 0)

    for layer in range(layers):
        def finish(g, carry):
            out_copy(layer, 0, g).wait()
            out_copy(layer, 1, g).wait()
            return carry

        lax.fori_loop(0, groups, finish, 0)
    hidden_copy.wait()


def write_caches(group, positions, hidden, knew, vnew, kbufs, vbufs, flat_shape):
    layers, batch, head = knew.shape
    groups = kbufs[0].shape[0]
    vm = pl.BlockSpec(memory_space=VMEM)
    hbm = pl.BlockSpec(memory_space=pltpu.HBM)
    caches = list(kbufs) + list(vbufs)
    dma = pltpu.SemaphoreType.DMA
    return pl.pallas_call(
        functools.partial(write_kernel, group, layers),
        out_shape=(jax.ShapeDtypeStruct(hidden.shape, BF16),) + (jax.ShapeDtypeStruct(flat_shape, BF16),) * 2 + tuple(VMEM(c.shape, BF16) for c in caches),
        in_specs=[hbm] + [vm] * (3 + len(caches)),
        out_specs=(hbm, hbm, hbm) + (vm,) * len(caches),
        scratch_shapes=[
            VMEM((layers, groups, head, group), F32),
            VMEM((layers, groups, head, group), F32),
            pltpu.SMEM((batch,), jnp.int32),
            dma,
            dma,
            dma((layers, 2, groups)),
        ],
        input_output_aliases={4 + n: 3 + n for n in range(len(caches))},
        compiler_params=pltpu.CompilerParams(vmem_limit_bytes=43 * 2**19),
        name='write_caches',
    )(*in_hbm([positions]), *in_vmem([hidden, knew, vnew] + caches))[:3]


def layers_kernel(layers, tp, group, cross_group, streams, *refs):
    refs = list(refs)
    counts = (2, len(VECTORS), len(WEIGHTS), 4, 3, layers, layers, 2, len(VECTORS), len(WEIGHTS))
    split = []
    for count in counts:
        split.append(refs[:count])
        del refs[:count]
    (pos_hbm, hidden_hbm), vec_hbm, weight_hbm, (kself_ref, vself_ref, kin_ref, vin_ref), (hidden_out_ref, knew_ref, vnew_ref), kselfs, vselfs, (pos_ref, hidden_ref), vec_refs, weight_refs = split
    gain_ref, bias_ref, bq_ref, bv_ref, bo_ref, bcq_ref, bco_ref, b1_ref, b2_ref = vec_refs
    wq_ref, wk_ref, wv_ref, wo_ref, wcq_ref, wco_ref, w1_ref, w2_ref = weight_refs
    (kbuf, vbuf, part, landed, blocks, gathered, packed, wide_w, qself, sself, oself, qbd, scores, param_sem, self_sem, in_sem, rs_send, rs_recv, ag_send, ag_recv, g_send, g_recv, w_send, w_recv) = refs
    me = lax.axis_index('tp')
    batch, width = hidden_ref.shape
    head = wcq_ref.shape[1]
    size = batch // streams
    half = size // 2
    quarters = width // 128
    scale = head ** -0.25
    groups, span, slots = kselfs[0].shape
    chunks, cross_span = kbuf.shape[:2]
    beams = batch // (chunks * cross_group)
    rows = cross_group * beams
    per_stream = chunks // streams
    peers = [lax.rem(me + step, tp) for step in sorted(range(1, tp), key=lambda step: abs(step - tp // 2))]
    same_core = [lax.rem(me + step, tp) for step in sorted(range(2, tp, 2), key=lambda step: abs(step - tp // 2))]
    sibling = me + 1 - 2 * lax.rem(me, 2)
    ids = range(streams)

    def remote(src, dst, send_sem, recv_sem, peer):
        return pltpu.make_async_remote_copy(src, dst, send_sem, recv_sem, device_id={'tp': peer}, device_id_type=pl.DeviceIdType.MESH)

    barrier = pltpu.get_barrier_semaphore()
    for peer in peers:
        pl.semaphore_signal(barrier, inc=1, device_id={'tp': peer}, device_id_type=pl.DeviceIdType.MESH)

    pairs = list(zip([pos_hbm, hidden_hbm] + vec_hbm + weight_hbm, [pos_ref, hidden_ref] + vec_refs + weight_refs))
    needed_first = 2 + len(vec_refs) + 3
    copies = load_all(pairs[:needed_first], param_sem)

    def self_copy(layer, which, g):
        src, dst = ((kself_ref, kselfs[layer]), (vself_ref, vselfs[layer]))[which]
        return pltpu.make_async_copy(src.at[pl.ds((layer * groups + g) * span, span), :], dst.at[g], self_sem.at[layer, which, g])

    def start_self(layer, which, s):
        def start(g, carry):
            self_copy(layer, which, g).start()
            return carry

        lax.fori_loop(s * (size // group), (s + 1) * (size // group), start, 0)

    def cross_copy(layer, which, c):
        src, buf = ((kin_ref, kbuf), (vin_ref, vbuf))[which]
        return pltpu.make_async_copy(src.at[pl.ds((layer * chunks + c) * cross_span, cross_span), :], buf.at[c], in_sem.at[layer, which, c])

    late_copies = [pltpu.make_async_copy(src, dst, param_sem.at[needed_first + n]) for n, (src, dst) in enumerate(pairs[needed_first:])]
    for copy in late_copies:
        copy.start()
    for s in ids:
        start_self(0, 0, s)
        start_self(0, 1, s)
    for copy in copies:
        copy.wait()
    sends = []

    def send(*args):
        copy = remote(*args)
        copy.start()
        sends.append(copy)

    def vec(ref, layer):
        return ref[layer:layer + 1, :].astype(F32)

    def norm(x, layer, k):
        return layer_norm(x, gain_ref[k, layer:layer + 1, :].astype(F32), bias_ref[k, layer:layer + 1, :].astype(F32))

    def bounds(j):
        r, c = j // quarters, j % quarters
        return slice(r * half, (r + 1) * half), slice(c * 128, (c + 1) * 128)

    def scatter(x, s, total, hidden):
        for j in range(tp):
            rs, cs = bounds(j)
            part[x, s, j] = total[rs, cs].astype(BF16)
            blocks[x, s, j] = hidden[rs, cs].astype(BF16)
        for n, peer in enumerate(peers):
            send(part.at[x, s, peer], landed.at[x, s, me], rs_send.at[x, s, n], rs_recv.at[x, s, me], peer)

    def reduce_and_gather(x, s, bias):
        own = lax.rem(me, quarters)
        bias_row = jnp.zeros((1, 128), F32)
        for c in range(quarters):
            bias_row = jnp.where(own == c, bias[:, c * 128:(c + 1) * 128], bias_row)
        for n, peer in reversed(list(enumerate(peers))):
            remote(part.at[x, s, peer], landed.at[x, s, peer], rs_send.at[x, s, n], rs_recv.at[x, s, peer], peer).wait_recv()
        acc = part[x, s, me].astype(F32) + blocks[x, s, me].astype(F32) + bias_row
        for peer in peers:
            acc = acc + landed[x, s, peer].astype(F32)
        blocks[x, s, me] = acc.astype(BF16)
        for n, peer in enumerate(peers):
            send(blocks.at[x, s, me], blocks.at[x, s, me], ag_send.at[x, s, n], ag_recv.at[x, s, me], peer)

    def collect(x, s):
        for n, peer in enumerate(peers):
            remote(blocks.at[x, s, peer], blocks.at[x, s, peer], ag_send.at[x, s, n], ag_recv.at[x, s, peer], peer).wait_recv()
        return jnp.concatenate([jnp.concatenate([blocks[x, s, r * quarters + c].astype(F32) for c in range(quarters)], axis=1) for r in range(tp // quarters)], axis=0)

    def share(x, s, vals):
        packed[x, s] = pack_half(vals)
        gathered[x, s, me] = packed[x, s]
        for n, peer in enumerate(peers):
            send(packed.at[x, s], gathered.at[x, s, me], g_send.at[x, s, n], g_recv.at[x, s, me], peer)

    def project_all(x, s, bias, hidden):
        for n, peer in enumerate(peers):
            remote(packed.at[x, s], gathered.at[x, s, peer], g_send.at[x, s, n], g_recv.at[x, s, peer], peer).wait_recv()
        vals = [gathered[x, s, j].astype(F32) for j in range(tp)]
        heads = jnp.concatenate([jnp.concatenate([v[:, :head] for v in vals], axis=1), jnp.concatenate([v[:, head:] for v in vals], axis=1)], axis=0)
        return (hidden + dot(heads.astype(BF16), wide_w[x].reshape(tp * head, width)) + bias).astype(BF16).astype(F32)

    def spread_weight(x):
        src = (wo_ref, wco_ref)[x % 2].at[x // 2]
        wide_w[x, me] = (wo_ref, wco_ref)[x % 2][x // 2]
        for n, peer in enumerate(same_core):
            send(src, wide_w.at[x, me], w_send.at[x, n], w_recv.at[x, me], peer)
        send(src, wide_w.at[x, me], w_send.at[x, tp // 2 - 1], w_recv.at[x, me], sibling)

    def forward_weight(x):
        for n, peer in enumerate(same_core):
            remote(wide_w.at[x, peer], wide_w.at[x, peer], w_send.at[x, n], w_recv.at[x, peer], peer).wait_recv()
            send(wide_w.at[x, peer], wide_w.at[x, peer], w_send.at[x, tp // 2 + n], w_recv.at[x, peer], sibling)

    def finish_weight(x):
        for step in range(0, tp, 2):
            origin = lax.rem(sibling + step, tp)
            remote(wide_w.at[x, origin], wide_w.at[x, origin], w_send.at[x, 0], w_recv.at[x, origin], sibling).wait_recv()

    self_batch = 5

    def self_attend(layer, s, hidden, after_projections):
        normed = norm(hidden, layer, 0)
        q = ((dot_nt(normed, wq_ref[layer]) + vec(bq_ref, layer)) * scale).astype(BF16)
        k = (dot_nt(normed, wk_ref[layer]) * scale).astype(BF16)
        v = (dot_nt(normed, wv_ref[layer]) + vec(bv_ref, layer)).astype(BF16)
        mine = slice(s * size, (s + 1) * size)
        knew_ref[layer, mine, :] = k
        vnew_ref[layer, mine, :] = v
        diag = iota((size, span), 0) % group == iota((size, span), 1) // head
        qself[...] = jnp.where(diag, repeat_lanes(q.astype(F32), span), 0.0)
        new_score = jnp.sum(q.astype(F32) * k.astype(F32), axis=-1, keepdims=True)
        after_projections()
        first_group = s * (size // group)

        count = size // group

        def score(g):
            limit = jnp.zeros((group, 1), jnp.int32)
            for i in range(group):
                limit = jnp.where(iota((group, 1), 0) == i, pos_ref[(first_group + g) * group + i], limit)
            raw = dot(qself[g * group:(g + 1) * group, :].astype(BF16), kselfs[layer][first_group + g])
            sself[g * group:(g + 1) * group, :] = jnp.where(iota((group, slots), 1) < limit, raw, NEG)

        def weigh(g):
            wide_o = dot_nt(vselfs[layer][first_group + g], sself[g * group:(g + 1) * group, :].astype(BF16))
            o_t = jnp.zeros((head, group), F32)
            for i in range(group):
                o_t = o_t + jnp.where(iota((head, group), 1) == i, wide_o[i * head:(i + 1) * head, :], 0.0)
            oself[g * group:(g + 1) * group, :] = o_t.T

        def batched(step, which):
            for n in range(0, count, self_batch):
                for g in range(n, n + self_batch):
                    self_copy(layer, which, first_group + g).wait()
                for g in range(n, n + self_batch):
                    step(g)

        batched(score, 0)
        raw = sself[...]
        top = jnp.maximum(jnp.max(raw, axis=-1, keepdims=True), new_score)
        probs = jnp.exp(raw - top)
        new_prob = jnp.exp(new_score - top)
        inv = 1.0 / (jnp.sum(probs, axis=-1, keepdims=True) + new_prob)
        sself[...] = probs * inv
        batched(weigh, 1)
        return oself[...] + (new_prob * inv).astype(BF16).astype(F32) * v.astype(F32)

    def cross_attend(layer, s, hidden):
        q = ((dot_nt(norm(hidden, layer, 1), wcq_ref[layer]) + vec(bcq_ref, layer)) * scale).astype(BF16)
        diag = (iota((size, cross_span), 0) // beams) % cross_group == iota((size, cross_span), 1) // head
        qbd[s] = jnp.where(diag, repeat_lanes(q.astype(F32), cross_span), 0.0).astype(BF16)
        for c in range(per_stream):
            cross_copy(layer, 0, s * per_stream + c).wait()
            cross_copy(layer, 1, s * per_stream + c).wait()
        for c in range(per_stream):
            scores[s, c * rows:(c + 1) * rows, :] = dot(qbd[s, c * rows:(c + 1) * rows, :], kbuf[s * per_stream + c])
        outs = []
        for c in range(per_stream):
            raw = scores[s, c * rows:(c + 1) * rows, :]
            probs = jnp.exp(raw - jnp.max(raw, axis=-1, keepdims=True))
            probs = (probs * (1.0 / jnp.sum(probs, axis=-1, keepdims=True))).astype(BF16)
            wide_o = dot_nt(vbuf[s * per_stream + c], probs)
            o_t = jnp.zeros((head, rows), F32)
            for i in range(cross_group):
                o_t = o_t + jnp.where(iota((head, rows), 1) // beams == i, wide_o[i * head:(i + 1) * head, :], 0.0)
            outs.append(o_t.T)
        return jnp.concatenate(outs, axis=0)

    def start_cross(layer, s):
        for c in range(s * per_stream, (s + 1) * per_stream):
            cross_copy(layer, 0, c).start()
            cross_copy(layer, 1, c).start()

    def mlp(layer, hidden):
        inner = dot(norm(hidden, layer, 2), w1_ref[layer]) + vec(b1_ref, layer)
        return dot((0.5 * inner * (1.0 + lax.erf(inner * (0.5 ** 0.5)))).astype(BF16), w2_ref[layer])

    def enter():
        for copy in late_copies:
            copy.wait()
        pl.semaphore_wait(barrier, tp - 1)
        spread_weight(0)

    states = [hidden_ref[s * size:(s + 1) * size, :].astype(F32) for s in ids]
    for layer in range(layers):
        early, late = 2 * layer, 2 * layer + 1
        for s in ids:
            if layer:
                states[s] = collect(layer - 1, s)
            begin = layer == 0 and s == 0
            share(early, s, self_attend(layer, s, states[s], enter if begin else lambda: None))
            if layer == 0:
                start_cross(0, s)
            if s == 0:
                spread_weight(late)
                if layer:
                    forward_weight(early)
        if layer == 0:
            forward_weight(early)
        if layer + 1 < layers:
            for s in ids:
                start_self(layer + 1, 0, s)
                start_self(layer + 1, 1, s)
        finish_weight(early)
        for s in ids:
            states[s] = project_all(early, s, vec(bo_ref, layer), states[s])
            share(late, s, cross_attend(layer, s, states[s]))
            if layer + 1 < layers:
                start_cross(layer + 1, s)
        forward_weight(late)
        finish_weight(late)
        for s in ids:
            states[s] = project_all(late, s, vec(bco_ref, layer), states[s])
            scatter(layer, s, mlp(layer, states[s]), states[s])
        for s in ids:
            reduce_and_gather(layer, s, vec(b2_ref, layer))
        if layer + 1 < layers:
            spread_weight(early + 2)
    for s in ids:
        hidden_out_ref[s * size:(s + 1) * size, :] = collect(layers - 1, s).astype(BF16)
    for copy in sends:
        copy.wait_send()


def run_layers(tp, group, cross_group, streams, hidden, positions, keys, vals, ckeys, cvals, params):
    batch, width = hidden.shape
    layers, head = params['w_cquery'].shape[:2]
    slots, frames = keys.shape[1], ckeys.shape[1]
    chunks = ckeys.shape[0] // layers // head // cross_group
    groups = batch // group
    size = batch // streams
    vm = pl.BlockSpec(memory_space=VMEM)
    hbm = pl.BlockSpec(memory_space=pltpu.HBM)
    operands = [positions, hidden] + [params[n] for n in VECTORS + WEIGHTS] + [keys, vals, ckeys, cvals]
    cache = VMEM((groups, group * head, slots), BF16)
    fresh = VMEM((layers, batch, head), BF16)
    block = (size // 2, 128)
    dma = pltpu.SemaphoreType.DMA
    hidden_out, knew, vnew, *caches = pl.pallas_call(
        functools.partial(layers_kernel, layers, tp, group, cross_group, streams),
        out_shape=(VMEM(hidden.shape, BF16), fresh, fresh) + (cache,) * (2 * layers),
        in_specs=[hbm] * len(operands),
        out_specs=(vm,) * (3 + 2 * layers),
        scratch_shapes=[pltpu.SMEM((batch,), jnp.int32), VMEM(hidden.shape, BF16)] + [VMEM(params[n].shape, BF16) for n in VECTORS + WEIGHTS] + [
            VMEM((chunks, cross_group * head, frames), BF16),
            VMEM((chunks, cross_group * head, frames), BF16),
            VMEM((layers, streams, tp) + block, BF16),
            VMEM((layers, streams, tp) + block, BF16),
            VMEM((layers, streams, tp) + block, BF16),
            VMEM((2 * layers, streams, tp) + block, BF16),
            VMEM((2 * layers, streams) + block, BF16),
            VMEM((2 * layers, tp) + params['w_out'].shape[1:], BF16),
            VMEM((size, group * head), F32),
            VMEM((size, slots), F32),
            VMEM((size, head), F32),
            VMEM((streams, size, cross_group * head), BF16),
            VMEM((streams, size, frames), F32),
            dma((2 + len(VECTORS) + len(WEIGHTS),)),
            dma((layers, 2, groups)),
            dma((layers, 2, chunks)),
            dma((layers, streams, tp - 1)),
            dma((layers, streams, tp)),
            dma((layers, streams, tp - 1)),
            dma((layers, streams, tp)),
            dma((2 * layers, streams, tp - 1)),
            dma((2 * layers, streams, tp)),
            dma((2 * layers, tp)),
            dma((2 * layers, tp)),
        ],
        compiler_params=pltpu.CompilerParams(vmem_limit_bytes=43 * 2**19, collective_id=0, has_side_effects=True),
        name='decoder_layers',
    )(*in_hbm(operands))
    return hidden_out, knew, vnew, caches[:layers], caches[layers:]


def solution(mesh):
    tp = mesh.shape['tp']
    cache_spec = P(None, 'dp', None, 'tp', None)
    col_spec = P(None, None, 'tp')
    row_spec = P(None, 'tp', None)
    vec_spec = P(None, 'tp')
    param_specs = {'ln_gain': P(), 'ln_bias': P(), 'w_query': col_spec, 'b_query': vec_spec, 'w_key': col_spec, 'w_value': col_spec, 'b_value': vec_spec, 'w_out': row_spec, 'b_out': P(), 'w_cquery': col_spec, 'b_cquery': vec_spec, 'w_cout': row_spec, 'b_cout': P(), 'w_fc1': col_spec, 'b_fc1': vec_spec, 'w_fc2': row_spec, 'b_fc2': P()}
    in_specs = (P('dp', None), P('dp'), cache_spec, cache_spec, cache_spec, cache_spec) + tuple(param_specs[param_name] for param_name in PARAM_NAMES)

    def flat(cache):
        layers, n, slots, heads, head = cache.shape
        return cache.transpose(0, 1, 3, 4, 2).reshape(layers * n * heads * head, slots)

    def local_step(hidden, positions, self_keys, self_vals, cross_keys, cross_vals, *layer_params):
        params = dict(zip(PARAM_NAMES, layer_params))
        for name in ('w_query', 'w_key', 'w_value', 'w_cquery'):
            params[name] = params[name].transpose(0, 2, 1)
        for name in ('ln_gain', 'ln_bias'):
            params[name] = params[name].transpose(1, 0, 2)
        layers, batch, slots, heads, head = self_keys.shape
        keys, vals, ckeys, cvals = flat(self_keys), flat(self_vals), flat(cross_keys), flat(cross_vals)
        streams, group, cross_group = 2, 8, 8
        hidden, knew, vnew, kbufs, vbufs = run_layers(tp, group, cross_group, streams, hidden, positions, keys, vals, ckeys, cvals, params)
        hidden, *outs = write_caches(group, positions, hidden, knew, vnew, kbufs, vbufs, keys.shape)

        def unflat(cache):
            return cache.reshape(layers, batch, heads, head, slots).transpose(0, 1, 4, 2, 3)

        return hidden, unflat(outs[0]), unflat(outs[1])

    return jax.shard_map(local_step, mesh=mesh, in_specs=in_specs, out_specs=(P('dp', None), cache_spec, cache_spec), check_vma=False)
```

```python
import functools

import jax
import jax.numpy as jnp
from jax import lax
from jax.experimental import pallas as pl
from jax.experimental.pallas import tpu as pltpu
from jax.sharding import PartitionSpec as P

EPS = 1e-5
NEG = -1e30
PARAM_NAMES = ('ln_gain', 'ln_bias', 'w_query', 'b_query', 'w_key', 'w_value', 'b_value', 'w_out', 'b_out', 'w_cquery', 'b_cquery', 'w_cout', 'b_cout', 'w_fc1', 'b_fc1', 'w_fc2', 'b_fc2')
F32 = jnp.float32
BF16 = jnp.bfloat16
VMEM = pltpu.VMEM
NT = (((1,), (1,)), ((), ()))


def dot(a, b):
    return jnp.dot(a, b, preferred_element_type=F32)


def dot_nt(a, b):
    return lax.dot_general(a, b, NT, preferred_element_type=F32)


def layer_norm(wide_vals, gain_row, bias_row):
    center = wide_vals - jnp.mean(wide_vals, axis=-1, keepdims=True)
    var_est = jnp.mean(center * center, axis=-1, keepdims=True)
    return (center * lax.rsqrt(var_est + EPS) * gain_row + bias_row).astype(BF16)


def repeat_lanes(vals, width):
    pair = jnp.concatenate([vals, vals], axis=1)
    return jnp.concatenate([pair] * (width // pair.shape[1]), axis=1)


def iota(shape, dim):
    return lax.broadcasted_iota(jnp.int32, shape, dim)


def load_all(pairs, sem):
    copies = [pltpu.make_async_copy(src, dst, sem.at[n]) for n, (src, dst) in enumerate(pairs)]
    for copy in copies:
        copy.start()
    return copies


def pack_half(vals):
    half = vals.shape[0] // 2
    return jnp.concatenate([vals[:half], vals[half:]], axis=1).astype(BF16)


def pack_half(vals):
    half = vals.shape[0] // 2
    return jnp.concatenate([vals[:half], vals[half:]], axis=1).astype(BF16)


def in_hbm(arrays):
    return [pltpu.with_memory_space_constraint(a, pltpu.HBM) for a in arrays]


def in_vmem(arrays):
    return [pltpu.with_memory_space_constraint(a, VMEM) for a in arrays]


VECTORS = ('ln_gain', 'ln_bias', 'b_query', 'b_value', 'b_out', 'b_cquery', 'b_cout', 'b_fc1', 'b_fc2')
WEIGHTS = ('w_query', 'w_key', 'w_value', 'w_out', 'w_cquery', 'w_cout', 'w_fc1', 'w_fc2')


def write_kernel(group, layers, pos_hbm, hidden_ref, knew_ref, vnew_ref, *refs):
    hidden_out_ref, kout_ref, vout_ref = refs[2 * layers:2 * layers + 3]
    kbufs = refs[2 * layers + 3:3 * layers + 3]
    vbufs = refs[3 * layers + 3:4 * layers + 3]
    kcol, vcol, pos_ref, pos_sem, hidden_sem, out_sem = refs[4 * layers + 3:]
    batch, head = knew_ref.shape[1:]
    groups, span, slots = kbufs[0].shape
    pos_copy = pltpu.make_async_copy(pos_hbm, pos_ref, pos_sem)
    pos_copy.start()
    hidden_copy = pltpu.make_async_copy(hidden_ref, hidden_out_ref, hidden_sem)
    hidden_copy.start()

    def out_copy(layer, which, g):
        buf, dst = ((kbufs[layer], kout_ref), (vbufs[layer], vout_ref))[which]
        return pltpu.make_async_copy(buf.at[g], dst.at[pl.ds((layer * groups + g) * span, span), :], out_sem.at[layer, which, g])

    full_tiles = slots // 128
    tail = slots - full_tiles * 128
    for layer in range(layers):
        k_t = knew_ref[layer].astype(F32).T
        v_t = vnew_ref[layer].astype(F32).T
        for g in range(groups):
            kcol[layer, g] = k_t[:, g * group:(g + 1) * group]
            vcol[layer, g] = v_t[:, g * group:(g + 1) * group]
        if layer == 0:
            pos_copy.wait()

        def update(g, carry):
            cols_of = (kcol[layer, g], vcol[layer, g])
            for i in range(group):
                pos = pos_ref[g * group + i]
                rows = slice(i * head, (i + 1) * head)
                first = pl.multiple_of(jnp.minimum(pos // 128, full_tiles - 1) * 128, 128)
                places = [(pl.ds(first, 128), iota((head, 128), 1) + first == pos)]
                if tail:
                    places.append((slice(full_tiles * 128, slots), iota((head, tail), 1) + full_tiles * 128 == pos))
                for cols, hit in places:
                    for buf, col in zip((kbufs[layer], vbufs[layer]), cols_of):
                        old = buf[g, rows, cols].astype(F32)
                        buf[g, rows, cols] = jnp.where(hit, col[:, i:i + 1], old).astype(BF16)
            out_copy(layer, 0, g).start()
            out_copy(layer, 1, g).start()
            return carry

        lax.fori_loop(0, groups, update, 0)

    for layer in range(layers):
        def finish(g, carry):
            out_copy(layer, 0, g).wait()
            out_copy(layer, 1, g).wait()
            return carry

        lax.fori_loop(0, groups, finish, 0)
    hidden_copy.wait()


def write_caches(group, positions, hidden, knew, vnew, kbufs, vbufs, flat_shape):
    layers, batch, head = knew.shape
    groups = kbufs[0].shape[0]
    vm = pl.BlockSpec(memory_space=VMEM)
    hbm = pl.BlockSpec(memory_space=pltpu.HBM)
    caches = list(kbufs) + list(vbufs)
    dma = pltpu.SemaphoreType.DMA
    return pl.pallas_call(
        functools.partial(write_kernel, group, layers),
        out_shape=(jax.ShapeDtypeStruct(hidden.shape, BF16),) + (jax.ShapeDtypeStruct(flat_shape, BF16),) * 2 + tuple(VMEM(c.shape, BF16) for c in caches),
        in_specs=[hbm] + [vm] * (3 + len(caches)),
        out_specs=(hbm, hbm, hbm) + (vm,) * len(caches),
        scratch_shapes=[
            VMEM((layers, groups, head, group), F32),
            VMEM((layers, groups, head, group), F32),
            pltpu.SMEM((batch,), jnp.int32),
            dma,
            dma,
            dma((layers, 2, groups)),
        ],
        input_output_aliases={4 + n: 3 + n for n in range(len(caches))},
        compiler_params=pltpu.CompilerParams(vmem_limit_bytes=43 * 2**19),
        name='write_caches',
    )(*in_hbm([positions]), *in_vmem([hidden, knew, vnew] + caches))[:3]


def layers_kernel(layers, tp, group, cross_group, streams, *refs):
    refs = list(refs)
    counts = (2, len(VECTORS), len(WEIGHTS), 4, 3, layers, layers, 2, len(VECTORS), len(WEIGHTS))
    split = []
    for count in counts:
        split.append(refs[:count])
        del refs[:count]
    (pos_hbm, hidden_hbm), vec_hbm, weight_hbm, (kself_ref, vself_ref, kin_ref, vin_ref), (hidden_out_ref, knew_ref, vnew_ref), kselfs, vselfs, (pos_ref, hidden_ref), vec_refs, weight_refs = split
    gain_ref, bias_ref, bq_ref, bv_ref, bo_ref, bcq_ref, bco_ref, b1_ref, b2_ref = vec_refs
    wq_ref, wk_ref, wv_ref, wo_ref, wcq_ref, wco_ref, w1_ref, w2_ref = weight_refs
    (kbuf, vbuf, part, landed, blocks, gathered, packed, wide_w, qself, sself, oself, qbd, scores, param_sem, self_sem, in_sem, rs_send, rs_recv, ag_send, ag_recv, g_send, g_recv, w_send, w_recv) = refs
    me = lax.axis_index('tp')
    batch, width = hidden_ref.shape
    head = wcq_ref.shape[1]
    size = batch // streams
    half = size // 2
    quarters = width // 128
    scale = head ** -0.25
    groups, span, slots = kselfs[0].shape
    chunks, cross_span = kbuf.shape[:2]
    beams = batch // (chunks * cross_group)
    rows = cross_group * beams
    per_stream = chunks // streams
    peers = [lax.rem(me + step, tp) for step in sorted(range(1, tp), key=lambda step: abs(step - tp // 2))]
    same_core = [lax.rem(me + step, tp) for step in sorted(range(2, tp, 2), key=lambda step: abs(step - tp // 2))]
    sibling = me + 1 - 2 * lax.rem(me, 2)
    ids = range(streams)

    def remote(src, dst, send_sem, recv_sem, peer):
        return pltpu.make_async_remote_copy(src, dst, send_sem, recv_sem, device_id={'tp': peer}, device_id_type=pl.DeviceIdType.MESH)

    barrier = pltpu.get_barrier_semaphore()
    for peer in peers:
        pl.semaphore_signal(barrier, inc=1, device_id={'tp': peer}, device_id_type=pl.DeviceIdType.MESH)

    pairs = list(zip([pos_hbm, hidden_hbm] + vec_hbm + weight_hbm, [pos_ref, hidden_ref] + vec_refs + weight_refs))
    needed_first = 2 + len(vec_refs) + 3
    copies = load_all(pairs[:needed_first], param_sem)

    def self_copy(layer, which, g):
        src, dst = ((kself_ref, kselfs[layer]), (vself_ref, vselfs[layer]))[which]
        return pltpu.make_async_copy(src.at[pl.ds((layer * groups + g) * span, span), :], dst.at[g], self_sem.at[layer, which, g])

    def start_self(layer, which, s):
        def start(g, carry):
            self_copy(layer, which, g).start()
            return carry

        lax.fori_loop(s * (size // group), (s + 1) * (size // group), start, 0)

    def cross_copy(layer, which, c):
        src, buf = ((kin_ref, kbuf), (vin_ref, vbuf))[which]
        return pltpu.make_async_copy(src.at[pl.ds((layer * chunks + c) * cross_span, cross_span), :], buf.at[c], in_sem.at[layer, which, c])

    late_copies = [pltpu.make_async_copy(src, dst, param_sem.at[needed_first + n]) for n, (src, dst) in enumerate(pairs[needed_first:])]
    for copy in late_copies:
        copy.start()
    for s in ids:
        start_self(0, 0, s)
        start_self(0, 1, s)
    for copy in copies:
        copy.wait()
    sends = []

    def send(*args):
        copy = remote(*args)
        copy.start()
        sends.append(copy)

    def vec(ref, layer):
        return ref[layer:layer + 1, :].astype(F32)

    def norm(x, layer, k):
        return layer_norm(x, gain_ref[k, layer:layer + 1, :].astype(F32), bias_ref[k, layer:layer + 1, :].astype(F32))

    def bounds(j):
        r, c = j // quarters, j % quarters
        return slice(r * half, (r + 1) * half), slice(c * 128, (c + 1) * 128)

    def scatter(x, s, total, hidden):
        for j in range(tp):
            rs, cs = bounds(j)
            part[x, s, j] = total[rs, cs].astype(BF16)
            blocks[x, s, j] = hidden[rs, cs].astype(BF16)
        for n, peer in enumerate(peers):
            send(part.at[x, s, peer], landed.at[x, s, me], rs_send.at[x, s, n], rs_recv.at[x, s, me], peer)

    def reduce_and_gather(x, s, bias):
        own = lax.rem(me, quarters)
        bias_row = jnp.zeros((1, 128), F32)
        for c in range(quarters):
            bias_row = jnp.where(own == c, bias[:, c * 128:(c + 1) * 128], bias_row)
        for n, peer in reversed(list(enumerate(peers))):
            remote(part.at[x, s, peer], landed.at[x, s, peer], rs_send.at[x, s, n], rs_recv.at[x, s, peer], peer).wait_recv()
        acc = part[x, s, me].astype(F32) + blocks[x, s, me].astype(F32) + bias_row
        for peer in peers:
            acc = acc + landed[x, s, peer].astype(F32)
        blocks[x, s, me] = acc.astype(BF16)
        for n, peer in enumerate(peers):
            send(blocks.at[x, s, me], blocks.at[x, s, me], ag_send.at[x, s, n], ag_recv.at[x, s, me], peer)

    def collect(x, s):
        for n, peer in enumerate(peers):
            remote(blocks.at[x, s, peer], blocks.at[x, s, peer], ag_send.at[x, s, n], ag_recv.at[x, s, peer], peer).wait_recv()
        return jnp.concatenate([jnp.concatenate([blocks[x, s, r * quarters + c].astype(F32) for c in range(quarters)], axis=1) for r in range(tp // quarters)], axis=0)

    def share(x, s, vals):
        packed[x, s] = pack_half(vals)
        gathered[x, s, me] = packed[x, s]
        for n, peer in enumerate(peers):
            send(packed.at[x, s], gathered.at[x, s, me], g_send.at[x, s, n], g_recv.at[x, s, me], peer)

    def project_all(x, s, bias, hidden):
        for n, peer in enumerate(peers):
            remote(packed.at[x, s], gathered.at[x, s, peer], g_send.at[x, s, n], g_recv.at[x, s, peer], peer).wait_recv()
        vals = [gathered[x, s, j].astype(F32) for j in range(tp)]
        heads = jnp.concatenate([jnp.concatenate([v[:, :head] for v in vals], axis=1), jnp.concatenate([v[:, head:] for v in vals], axis=1)], axis=0)
        return (hidden + dot(heads.astype(BF16), wide_w[x].reshape(tp * head, width)) + bias).astype(BF16).astype(F32)

    def spread_weight(x):
        src = (wo_ref, wco_ref)[x % 2].at[x // 2]
        wide_w[x, me] = (wo_ref, wco_ref)[x % 2][x // 2]
        for n, peer in enumerate(same_core):
            send(src, wide_w.at[x, me], w_send.at[x, n], w_recv.at[x, me], peer)
        send(src, wide_w.at[x, me], w_send.at[x, tp // 2 - 1], w_recv.at[x, me], sibling)

    def forward_weight(x):
        for n, peer in enumerate(same_core):
            remote(wide_w.at[x, peer], wide_w.at[x, peer], w_send.at[x, n], w_recv.at[x, peer], peer).wait_recv()
            send(wide_w.at[x, peer], wide_w.at[x, peer], w_send.at[x, tp // 2 + n], w_recv.at[x, peer], sibling)

    def finish_weight(x):
        for step in range(0, tp, 2):
            origin = lax.rem(sibling + step, tp)
            remote(wide_w.at[x, origin], wide_w.at[x, origin], w_send.at[x, 0], w_recv.at[x, origin], sibling).wait_recv()

    self_batch = 5

    def self_attend(layer, s, hidden, after_projections):
        normed = norm(hidden, layer, 0)
        q = ((dot_nt(normed, wq_ref[layer]) + vec(bq_ref, layer)) * scale).astype(BF16)
        k = (dot_nt(normed, wk_ref[layer]) * scale).astype(BF16)
        v = (dot_nt(normed, wv_ref[layer]) + vec(bv_ref, layer)).astype(BF16)
        mine = slice(s * size, (s + 1) * size)
        knew_ref[layer, mine, :] = k
        vnew_ref[layer, mine, :] = v
        diag = iota((size, span), 0) % group == iota((size, span), 1) // head
        qself[...] = jnp.where(diag, repeat_lanes(q.astype(F32), span), 0.0)
        new_score = jnp.sum(q.astype(F32) * k.astype(F32), axis=-1, keepdims=True)
        after_projections()
        first_group = s * (size // group)

        count = size // group

        def score(g):
            limit = jnp.zeros((group, 1), jnp.int32)
            for i in range(group):
                limit = jnp.where(iota((group, 1), 0) == i, pos_ref[(first_group + g) * group + i], limit)
            raw = dot(qself[g * group:(g + 1) * group, :].astype(BF16), kselfs[layer][first_group + g])
            sself[g * group:(g + 1) * group, :] = jnp.where(iota((group, slots), 1) < limit, raw, NEG)

        def weigh(g):
            wide_o = dot_nt(vselfs[layer][first_group + g], sself[g * group:(g + 1) * group, :].astype(BF16))
            o_t = jnp.zeros((head, group), F32)
            for i in range(group):
                o_t = o_t + jnp.where(iota((head, group), 1) == i, wide_o[i * head:(i + 1) * head, :], 0.0)
            oself[g * group:(g + 1) * group, :] = o_t.T

        def batched(step, which):
            for n in range(0, count, self_batch):
                for g in range(n, n + self_batch):
                    self_copy(layer, which, first_group + g).wait()
                for g in range(n, n + self_batch):
                    step(g)

        batched(score, 0)
        raw = sself[...]
        top = jnp.maximum(jnp.max(raw, axis=-1, keepdims=True), new_score)
        probs = jnp.exp(raw - top)
        new_prob = jnp.exp(new_score - top)
        inv = 1.0 / (jnp.sum(probs, axis=-1, keepdims=True) + new_prob)
        sself[...] = probs * inv
        batched(weigh, 1)
        return oself[...] + (new_prob * inv).astype(BF16).astype(F32) * v.astype(F32)

    def cross_attend(layer, s, hidden):
        q = ((dot_nt(norm(hidden, layer, 1), wcq_ref[layer]) + vec(bcq_ref, layer)) * scale).astype(BF16)
        diag = (iota((size, cross_span), 0) // beams) % cross_group == iota((size, cross_span), 1) // head
        qbd[s] = jnp.where(diag, repeat_lanes(q.astype(F32), cross_span), 0.0).astype(BF16)
        for c in range(per_stream):
            cross_copy(layer, 0, s * per_stream + c).wait()
            cross_copy(layer, 1, s * per_stream + c).wait()
        for c in range(per_stream):
            scores[s, c * rows:(c + 1) * rows, :] = dot(qbd[s, c * rows:(c + 1) * rows, :], kbuf[s * per_stream + c])
        outs = []
        for c in range(per_stream):
            raw = scores[s, c * rows:(c + 1) * rows, :]
            probs = jnp.exp(raw - jnp.max(raw, axis=-1, keepdims=True))
            probs = (probs * (1.0 / jnp.sum(probs, axis=-1, keepdims=True))).astype(BF16)
            wide_o = dot_nt(vbuf[s * per_stream + c], probs)
            o_t = jnp.zeros((head, rows), F32)
            for i in range(cross_group):
                o_t = o_t + jnp.where(iota((head, rows), 1) // beams == i, wide_o[i * head:(i + 1) * head, :], 0.0)
            outs.append(o_t.T)
        return jnp.concatenate(outs, axis=0)

    def start_cross(layer, s):
        for c in range(s * per_stream, (s + 1) * per_stream):
            cross_copy(layer, 0, c).start()
            cross_copy(layer, 1, c).start()

    def mlp(layer, hidden):
        inner = dot(norm(hidden, layer, 2), w1_ref[layer]) + vec(b1_ref, layer)
        return dot((0.5 * inner * (1.0 + lax.erf(inner * (0.5 ** 0.5)))).astype(BF16), w2_ref[layer])

    def enter():
        for copy in late_copies:
            copy.wait()
        pl.semaphore_wait(barrier, tp - 1)
        spread_weight(0)

    states = [hidden_ref[s * size:(s + 1) * size, :].astype(F32) for s in ids]
    for layer in range(layers):
        early, late = 2 * layer, 2 * layer + 1
        for s in ids:
            if layer:
                states[s] = collect(layer - 1, s)
            begin = layer == 0 and s == 0
            share(early, s, self_attend(layer, s, states[s], enter if begin else lambda: None))
            if layer == 0:
                start_cross(0, s)
            if s == 0:
                spread_weight(late)
        forward_weight(early)
        if layer + 1 < layers:
            for s in ids:
                start_self(layer + 1, 0, s)
                start_self(layer + 1, 1, s)
        finish_weight(early)
        for s in ids:
            states[s] = project_all(early, s, vec(bo_ref, layer), states[s])
            share(late, s, cross_attend(layer, s, states[s]))
            if layer + 1 < layers:
                start_cross(layer + 1, s)
        forward_weight(late)
        finish_weight(late)
        for s in ids:
            states[s] = project_all(late, s, vec(bco_ref, layer), states[s])
            scatter(layer, s, mlp(layer, states[s]), states[s])
        for s in ids:
            reduce_and_gather(layer, s, vec(b2_ref, layer))
        if layer + 1 < layers:
            spread_weight(early + 2)
    for s in ids:
        hidden_out_ref[s * size:(s + 1) * size, :] = collect(layers - 1, s).astype(BF16)
    for copy in sends:
        copy.wait_send()


def run_layers(tp, group, cross_group, streams, hidden, positions, keys, vals, ckeys, cvals, params):
    batch, width = hidden.shape
    layers, head = params['w_cquery'].shape[:2]
    slots, frames = keys.shape[1], ckeys.shape[1]
    chunks = ckeys.shape[0] // layers // head // cross_group
    groups = batch // group
    size = batch // streams
    vm = pl.BlockSpec(memory_space=VMEM)
    hbm = pl.BlockSpec(memory_space=pltpu.HBM)
    operands = [positions, hidden] + [params[n] for n in VECTORS + WEIGHTS] + [keys, vals, ckeys, cvals]
    cache = VMEM((groups, group * head, slots), BF16)
    fresh = VMEM((layers, batch, head), BF16)
    block = (size // 2, 128)
    dma = pltpu.SemaphoreType.DMA
    hidden_out, knew, vnew, *caches = pl.pallas_call(
        functools.partial(layers_kernel, layers, tp, group, cross_group, streams),
        out_shape=(VMEM(hidden.shape, BF16), fresh, fresh) + (cache,) * (2 * layers),
        in_specs=[hbm] * len(operands),
        out_specs=(vm,) * (3 + 2 * layers),
        scratch_shapes=[pltpu.SMEM((batch,), jnp.int32), VMEM(hidden.shape, BF16)] + [VMEM(params[n].shape, BF16) for n in VECTORS + WEIGHTS] + [
            VMEM((chunks, cross_group * head, frames), BF16),
            VMEM((chunks, cross_group * head, frames), BF16),
            VMEM((layers, streams, tp) + block, BF16),
            VMEM((layers, streams, tp) + block, BF16),
            VMEM((layers, streams, tp) + block, BF16),
            VMEM((2 * layers, streams, tp) + block, BF16),
            VMEM((2 * layers, streams) + block, BF16),
            VMEM((2 * layers, tp) + params['w_out'].shape[1:], BF16),
            VMEM((size, group * head), F32),
            VMEM((size, slots), F32),
            VMEM((size, head), F32),
            VMEM((streams, size, cross_group * head), BF16),
            VMEM((streams, size, frames), F32),
            dma((2 + len(VECTORS) + len(WEIGHTS),)),
            dma((layers, 2, groups)),
            dma((layers, 2, chunks)),
            dma((layers, streams, tp - 1)),
            dma((layers, streams, tp)),
            dma((layers, streams, tp - 1)),
            dma((layers, streams, tp)),
            dma((2 * layers, streams, tp - 1)),
            dma((2 * layers, streams, tp)),
            dma((2 * layers, tp)),
            dma((2 * layers, tp)),
        ],
        compiler_params=pltpu.CompilerParams(vmem_limit_bytes=43 * 2**19, collective_id=0, has_side_effects=True),
        name='decoder_layers',
    )(*in_hbm(operands))
    return hidden_out, knew, vnew, caches[:layers], caches[layers:]


def solution(mesh):
    tp = mesh.shape['tp']
    cache_spec = P(None, 'dp', None, 'tp', None)
    col_spec = P(None, None, 'tp')
    row_spec = P(None, 'tp', None)
    vec_spec = P(None, 'tp')
    param_specs = {'ln_gain': P(), 'ln_bias': P(), 'w_query': col_spec, 'b_query': vec_spec, 'w_key': col_spec, 'w_value': col_spec, 'b_value': vec_spec, 'w_out': row_spec, 'b_out': P(), 'w_cquery': col_spec, 'b_cquery': vec_spec, 'w_cout': row_spec, 'b_cout': P(), 'w_fc1': col_spec, 'b_fc1': vec_spec, 'w_fc2': row_spec, 'b_fc2': P()}
    in_specs = (P('dp', None), P('dp'), cache_spec, cache_spec, cache_spec, cache_spec) + tuple(param_specs[param_name] for param_name in PARAM_NAMES)

    def flat(cache):
        layers, n, slots, heads, head = cache.shape
        return cache.transpose(0, 1, 3, 4, 2).reshape(layers * n * heads * head, slots)

    def local_step(hidden, positions, self_keys, self_vals, cross_keys, cross_vals, *layer_params):
        params = dict(zip(PARAM_NAMES, layer_params))
        for name in ('w_query', 'w_key', 'w_value', 'w_cquery'):
            params[name] = params[name].transpose(0, 2, 1)
        for name in ('ln_gain', 'ln_bias'):
            params[name] = params[name].transpose(1, 0, 2)
        layers, batch, slots, heads, head = self_keys.shape
        keys, vals, ckeys, cvals = flat(self_keys), flat(self_vals), flat(cross_keys), flat(cross_vals)
        streams, group, cross_group = 2, 8, 8
        hidden, knew, vnew, kbufs, vbufs = run_layers(tp, group, cross_group, streams, hidden, positions, keys, vals, ckeys, cvals, params)
        hidden, *outs = write_caches(group, positions, hidden, knew, vnew, kbufs, vbufs, keys.shape)

        def unflat(cache):
            return cache.reshape(layers, batch, heads, head, slots).transpose(0, 1, 4, 2, 3)

        return hidden, unflat(outs[0]), unflat(outs[1])

    return jax.shard_map(local_step, mesh=mesh, in_specs=in_specs, out_specs=(P('dp', None), cache_spec, cache_spec), check_vma=False)
```
